128 devices in a mesh: owner: 4 (over y_lo, core), rows: 32 (over z, y_hi, x).
Axes of the slice: x: 4, y: 4 (y_hi: 2, y_lo: 2; y = y_hi * 2 + y_lo), z: 4, core: 2. Of those that a mesh axis runs over, the one named last changes fastest.
Arguments:
- w_gate: float32 [64, 2048, 1024], P('owner', 'rows'), may hold values from -0.25 to 0.25
- avg_gate: float32 [64, 2048, 1024], P('owner', 'rows'), may hold values from -0.125 to 0.125
- w_up: float32 [64, 2048, 1024], P('owner', 'rows'), may hold values from -0.25 to 0.25
- avg_up: float32 [64, 2048, 1024], P('owner', 'rows'), may hold values from -0.125 to 0.125
- mix_share: float32 [64], P('owner'), may hold values from 0.2 to 0.8
- router_weight: float32 [2048, 64], P('rows', 'owner'), may hold values from -0.125 to 0.125
- router_gain: float32 [2048], P('rows'), may hold values from 0.25 to 1.75
Outputs:
- serve_gate: bfloat16 [64, 2048, 1024], P('owner', None, 'rows')
- serve_up: bfloat16 [64, 2048, 1024], P('owner', None, 'rows')
- scale_gate: float32 [64, 1024], P('owner', 'rows')
- scale_up: float32 [64, 1024], P('owner', 'rows')
- serve_router: bfloat16 [2048, 64], replicated
The draws below stay inside these ranges and needn't reach their ends.
All inputs are finite; a program needn't handle non-finite values.
Results may differ from the reference program's by a relative error of at most 0.001.
Values may be sent and summed in bfloat16 or wider, within the bound.
A program may use at most 128 MiB of HBM per device.

```python
import jax
import jax.numpy as jnp
from jax import lax

EXPERTS = 64
D_MODEL = 2048
D_EXPERT = 1024


def raised(array, key, source, target, parts, factor):
    owner, partner = [(jnp.arange(array.shape[position]) // (array.shape[position] // parts)).reshape([-1 if axis == position else 1 for axis in range(array.ndim)]) for position in (source, target)]
    chosen = jax.random.permutation(key, parts)[partner]
    strong = (owner == chosen) | (owner == (partner + parts // 2) % parts)
    return jnp.where(strong, factor * array, array)


def levels(key, dims, split, smallest, high):
    def one(dim, blocks):
        steps = jax.random.uniform(jax.random.fold_in(jax.random.fold_in(key, 6), dim), (blocks,), jnp.float32, smallest / len(split), high / len(split))
        return jnp.repeat(jnp.exp(steps), dims[dim] // blocks).reshape((-1,) + (1,) * (len(dims) - dim - 1))

    level = one(*split[0])
    for cut in split[1:]:
        level = level * one(*cut)
    return level


def scatter_about(rng, extent, deviation, most, split=(), kind=jnp.bfloat16):
    gain = levels(rng, extent, split, -0.22, 0.18) if split else 1.0
    result = jax.random.normal(rng, extent, jnp.float32) * deviation * gain
    return jnp.minimum(jnp.maximum(result, -most), most).astype(kind)


def noise_with(stream_key, dims, spread, reach, shards, heavy, dtype=jnp.bfloat16):
    entries = spread * jax.random.normal(stream_key, dims, jnp.float32)
    if shards:
        entries = entries * levels(stream_key, dims, shards, -0.22, 0.18)
    return jnp.clip(raised(entries, jax.random.fold_in(stream_key, 3), *heavy), -reach, reach).astype(dtype)


def setup_inputs(seed: int = 0) -> dict:
    seeds = jax.random.split(jax.random.key(seed), 8)
    w_gate = noise_with(seeds[0], (EXPERTS, D_MODEL, D_EXPERT), D_MODEL ** -0.5, 0.25, ((0, 4), (1, 32)), (1, 2, 32, 2.75), jnp.float32)
    avg_gate = scatter_about(seeds[1], (EXPERTS, D_MODEL, D_EXPERT), D_MODEL ** -0.5, 0.125, ((0, 4), (1, 32)), jnp.float32)
    w_up = noise_with(seeds[2], (EXPERTS, D_MODEL, D_EXPERT), D_MODEL ** -0.5, 0.25, ((0, 4), (1, 32)), (1, 2, 32, 2.75), jnp.float32)
    avg_up = scatter_about(seeds[3], (EXPERTS, D_MODEL, D_EXPERT), D_MODEL ** -0.5, 0.125, ((0, 4), (1, 32)), jnp.float32)
    mix_share = jnp.clip(0.2 + 0.6 * jax.random.uniform(seeds[4], (EXPERTS,), jnp.float32) ** levels(seeds[4], (EXPERTS,), ((0, 4),), -0.2, 0.2), 0.2, 0.8)
    router_weight = scatter_about(seeds[5], (D_MODEL, EXPERTS), D_MODEL ** -0.5, 0.125, ((0, 32), (1, 4)), jnp.float32)
    router_gain = jnp.clip(1.0 + 0.15 * jax.random.normal(seeds[6], (D_MODEL,), jnp.float32), 0.25, 1.75)
    return dict(w_gate=w_gate, avg_gate=avg_gate, w_up=w_up, avg_up=avg_up, mix_share=mix_share, router_weight=router_weight, router_gain=router_gain)


def reference(w_gate, avg_gate, w_up, avg_up, mix_share, router_weight, router_gain):
    fresh_gate = mix_share[:, None, None] * w_gate + (1.0 - mix_share[:, None, None]) * avg_gate
    fresh_up = mix_share[:, None, None] * w_up + (1.0 - mix_share[:, None, None]) * avg_up
    scale_gate = jnp.sqrt(lax.optimization_barrier(jnp.sum(fresh_gate * fresh_gate, axis=1)))
    serve_gate = (fresh_gate / jnp.expand_dims(scale_gate, 1)).astype(jnp.bfloat16)
    scale_up = jnp.sqrt(lax.optimization_barrier(jnp.sum(fresh_up * fresh_up, axis=1)))
    serve_up = (fresh_up / jnp.expand_dims(scale_up, 1)).astype(jnp.bfloat16)
    serve_router = (router_weight * router_gain[:, None]).astype(jnp.bfloat16)
    return (serve_gate, serve_up, scale_gate, scale_up, serve_router)
```

```python
import functools

import jax
import jax.numpy as jnp
from jax import lax
from jax.experimental import pallas as pl
from jax.experimental.pallas import tpu as pltpu
from jax.sharding import PartitionSpec as P

MESH = pl.DeviceIdType.MESH
SPAN = 252.0
LOW = 125.0
OFFSETS = [(a, b, c) for a in range(4) for b in range(2) for c in range(4)][1:]
NEAREST = sorted(OFFSETS, key=lambda o: min(o[0], 4 - o[0]) + 2 * o[1] + min(o[2], 4 - o[2]))


def left_half(shape):
    return lax.broadcasted_iota(jnp.int32, shape, len(shape) - 1) < 64


def swap_halves(a, b):
    left = left_half(a.shape)
    return jnp.where(left, a, pltpu.roll(b, 64, 1)), jnp.where(left, pltpu.roll(a, 64, 1), b)


def exchange(
    mix, w_gate, v_gate, w_up, v_up, weight, gain,
    out_gate, out_up, out_scale, out_router,
    w_in, v_in, peaks, sent, landed, sent_side, landed_side, side, spread, mixed, lines, scales,
    in_sem, send_sem, recv_sem, side_send, side_recv, line_send, line_recv,
):
    me, own = lax.axis_index("rows"), lax.axis_index("owner")
    z, y, x = me // 8, (me // 4) % 2, me % 4
    peers = [((z + a) % 4) * 8 + ((y + b) % 2) * 4 + (x + c) % 4 for a, b, c in NEAREST]
    sources = ((w_gate, v_gate), (w_up, v_up))

    def arrival(m, p, k):
        return pltpu.make_async_copy(
            sources[m][k].at[pl.ds(2 * p, 2)],
            (w_in, v_in)[k].at[m, pl.ds(2 * p, 2)],
            in_sem.at[m, p, k],
        )

    for m in range(2):
        for p in range(8):
            for k in range(2):
                arrival(m, p, k).start()

    barrier = pltpu.get_barrier_semaphore()
    for peer in peers:
        pl.semaphore_signal(barrier, inc=1, device_id=(own, peer), device_id_type=MESH)
    for step in range(1, 4):
        pl.semaphore_signal(
            barrier, inc=1, device_id=((own + step) % 4, me), device_id_type=MESH
        )

    for m in range(2):

        def code(p, carry, m=m):
            for k in range(2):
                arrival(m, p, k).wait()
            for q in range(8):
                cols = pl.ds(128 * q, 128)
                halves = []
                for h in range(2):
                    e = 2 * p + h
                    share = mix[e]
                    f = share * w_in[m, e, :, cols] + (1.0 - share) * v_in[m, e, :, cols]
                    size = jnp.abs(f)
                    peak = jnp.max(size, axis=0, keepdims=True)
                    peak = (peak * (1.0 + 2.0**-7)).astype(jnp.bfloat16).astype(jnp.float32)
                    peaks[16 * m + e, :, cols] = peak
                    rate = jnp.where(peak > 1e-30, SPAN / peak, 0.0)
                    level = jnp.exp2(size * rate - LOW)
                    halves.append(jnp.where(f < 0, -level, level))
                block = jnp.concatenate(halves, axis=0).T.astype(jnp.bfloat16)
                for r in range(4):
                    sent[8 * m + p, 4 * q + r] = block[32 * r : 32 * r + 32]
            landed[8 * m + p, me] = sent[8 * m + p, me]
            return carry

        lax.fori_loop(0, 8, code, 0)

    group = lax.broadcasted_iota(jnp.int32, (8, 128), 1) // 32
    routed = weight[...] * gain[...]
    routed = jnp.concatenate([routed[:8], routed[8:]], axis=1)
    for q in range(8):
        blocks = [peaks[8 * k : 8 * k + 8, 0, 128 * q : 128 * q + 128] for k in range(4)]
        for r in range(4):
            turned = blocks[r]
            for k in range(4):
                if k != r:
                    turned = jnp.where(
                        group == k, pltpu.roll(blocks[k], (32 * (k - r)) % 128, 1), turned
                    )
            sent_side[4 * q + r] = jnp.concatenate([turned, routed], axis=0).astype(jnp.bfloat16)
    landed_side[me] = sent_side[me]

    pl.semaphore_wait(barrier, 34)

    for peer in peers:
        pltpu.make_async_remote_copy(
            src_ref=sent_side.at[peer], dst_ref=landed_side.at[me],
            send_sem=side_send, recv_sem=side_recv,
            device_id=(own, peer), device_id_type=MESH,
        ).start()

    def ship(c, carry):
        for peer in peers:
            pltpu.make_async_remote_copy(
                src_ref=sent.at[c, peer], dst_ref=landed.at[c, me],
                send_sem=send_sem.at[c], recv_sem=recv_sem.at[c],
                device_id=(own, peer), device_id_type=MESH,
            ).start()
        return carry

    lax.fori_loop(0, 16, ship, 0)

    def all_side():
        return pltpu.make_async_remote_copy(
            src_ref=sent_side.at[pl.ds(0, 31)], dst_ref=landed_side.at[pl.ds(0, 31)],
            send_sem=side_send, recv_sem=side_recv, device_id=(own, peers[0]), device_id_type=MESH,
        )

    def all_codes(c):
        return pltpu.make_async_remote_copy(
            src_ref=sent.at[c, pl.ds(0, 31)], dst_ref=landed.at[c, pl.ds(0, 31)],
            send_sem=send_sem.at[c], recv_sem=recv_sem.at[c],
            device_id=(own, peers[0]), device_id_type=MESH,
        )

    all_side().wait_recv()
    side[...] = landed_side[...].astype(jnp.float32)

    for k in range(16):
        for h, block in enumerate(swap_halves(side[2 * k, 8:, :], side[2 * k + 1, 8:, :])):
            lines[own, 8 * h : 8 * h + 8, 128 * k : 128 * k + 128] = block.astype(jnp.bfloat16)

    def pass_on(step):
        return pltpu.make_async_remote_copy(
            src_ref=lines.at[own], dst_ref=lines.at[own],
            send_sem=line_send.at[step - 1], recv_sem=line_recv.at[step - 1],
            device_id=((own + step) % 4, me), device_id_type=MESH,
        )

    for step in range(1, 4):
        pass_on(step).start()

    at = lax.broadcasted_iota(jnp.int32, (32, 2048), 1) // 64
    picks = (at == lax.broadcasted_iota(jnp.int32, (32, 2048), 0)).astype(jnp.bfloat16)
    for r in range(8):
        turned = side[:, r, :].T.astype(jnp.bfloat16)
        spread[r] = jnp.dot(turned, picks, preferred_element_type=jnp.float32)

    scales[...] = jnp.zeros_like(scales)
    for m, out in enumerate((out_gate, out_up)):

        def decode(p, carry, m=m, out=out):
            c = 8 * m + p
            all_codes(c).wait_recv()
            rows = []
            for h in range(2):
                e = 2 * p + h
                rows.append((e % 8, pl.ds(pl.multiple_of(32 * (2 * m + e // 8), 32), 32)))
            sums = [jnp.zeros((32, 128), jnp.float32)] * 2
            for k in range(16):
                levels = []
                for s in range(2):
                    block = landed[c, 2 * k + s].astype(jnp.float32)
                    size = jnp.log2(jnp.abs(block)) + LOW
                    levels.append(jnp.where(block < 0, -size, size))
                for h, level in enumerate(swap_halves(*levels)):
                    f = level * spread[rows[h][0], rows[h][1], 128 * k : 128 * k + 128]
                    sums[h] += f * f
                    mixed[h, :, 128 * k : 128 * k + 128] = f
            lane = lax.broadcasted_iota(jnp.int32, (32, 128), 1)
            for h in range(2):
                e = 2 * p + h
                scale = jnp.sqrt(jnp.sum(sums[h], axis=1, keepdims=True))
                scales[...] = jnp.where(lane == 16 * m + e, scale * (1.0 / SPAN), scales[...])
                out[e] = (mixed[h] * (1.0 / scale)).astype(jnp.bfloat16)
            return carry

        lax.fori_loop(0, 8, decode, 0)

    out_scale[...] = scales[...].T[:32]

    for step in range(1, 4):
        pass_on(step).wait()
    for o in range(4):
        out_router[16 * o : 16 * o + 16] = lines[o]

    all_side().wait_send()

    def drain(c, carry):
        all_codes(c).wait_send()
        return carry

    lax.fori_loop(0, 16, drain, 0)


def body(w_gate, avg_gate, w_up, avg_up, mix_share, router_weight, router_gain):
    vmem = pl.BlockSpec(memory_space=pltpu.VMEM)
    hbm = pl.BlockSpec(memory_space=pl.ANY)
    f32, bf16 = jnp.float32, jnp.bfloat16
    serve_gate, serve_up, scale, router = pl.pallas_call(
        exchange,
        out_shape=[
            jax.ShapeDtypeStruct((16, 32, 2048), bf16),
            jax.ShapeDtypeStruct((16, 32, 2048), bf16),
            jax.ShapeDtypeStruct((32, 32), f32),
            jax.ShapeDtypeStruct((64, 2048), bf16),
        ],
        in_specs=[pl.BlockSpec(memory_space=pltpu.SMEM), hbm, hbm, hbm, hbm, vmem, vmem],
        out_specs=[vmem] * 4,
        scratch_shapes=[
            pltpu.VMEM((2, 16, 64, 1024), f32),
            pltpu.VMEM((2, 16, 64, 1024), f32),
            pltpu.VMEM((32, 1, 1024), f32),
            pltpu.VMEM((16, 32, 32, 128), bf16),
            pltpu.VMEM((16, 32, 32, 128), bf16),
            pltpu.VMEM((32, 16, 128), bf16),
            pltpu.VMEM((32, 16, 128), bf16),
            pltpu.VMEM((32, 16, 128), f32),
            pltpu.VMEM((8, 128, 2048), f32),
            pltpu.VMEM((2, 32, 2048), f32),
            pltpu.VMEM((4, 16, 2048), bf16),
            pltpu.VMEM((32, 128), f32),
            pltpu.SemaphoreType.DMA((2, 8, 2)),
            pltpu.SemaphoreType.DMA((16,)),
            pltpu.SemaphoreType.DMA((16,)),
            pltpu.SemaphoreType.DMA,
            pltpu.SemaphoreType.DMA,
            pltpu.SemaphoreType.DMA((3,)),
            pltpu.SemaphoreType.DMA((3,)),
        ],
        compiler_params=pltpu.CompilerParams(
            collective_id=0, has_side_effects=True, vmem_limit_bytes=56 << 20
        ),
        name="exchange",
    )(
        mix_share, w_gate, avg_gate, w_up, avg_up, router_weight.T, router_gain.reshape(1, 64)
    )
    return (
        jnp.swapaxes(serve_gate, 1, 2),
        jnp.swapaxes(serve_up, 1, 2),
        scale[:16],
        scale[16:],
        router.T,
    )


def solution(mesh):
    return jax.shard_map(
        body,
        mesh=mesh,
        in_specs=(
            P("owner", "rows", None),
            P("owner", "rows", None),
            P("owner", "rows", None),
            P("owner", "rows", None),
            P("owner"),
            P("rows", "owner"),
            P("rows"),
        ),
        out_specs=(
            P("owner", None, "rows"),
            P("owner", None, "rows"),
            P("owner", "rows"),
            P("owner", "rows"),
            P(),
        ),
        check_vma=False,
    )
```

```python
import functools

import jax
import jax.numpy as jnp
from jax import lax
from jax.experimental import pallas as pl
from jax.experimental.pallas import tpu as pltpu
from jax.sharding import PartitionSpec as P

MESH = pl.DeviceIdType.MESH
SPAN = 252.0
LOW = 125.0
AHEAD = 4
FIRST = 4
SECOND = 12
OFFSETS = [(a, b, c) for a in range(4) for b in range(2) for c in range(4)][1:]
NEAREST = sorted(OFFSETS, key=lambda o: min(o[0], 4 - o[0]) + 2 * o[1] + min(o[2], 4 - o[2]))


def left_half(shape):
    return lax.broadcasted_iota(jnp.int32, shape, len(shape) - 1) < 64


def swap_halves(a, b):
    left = left_half(a.shape)
    return jnp.where(left, a, pltpu.roll(b, 64, 1)), jnp.where(left, pltpu.roll(a, 64, 1), b)


def exchange(
    mix_hbm, w_gate, v_gate, w_up, v_up, weight_hbm, gain_hbm,
    out_gate, out_up, out_scale_gate, out_scale_up, out_router,
    mix, weight, gain, w_in, v_in, peaks, sent, landed, sent_side, landed_side, side, spread, mixed, lines, scales,
    small_sem, in_sem, send_sem, recv_sem, side_send, side_recv, line_send, line_recv,
):
    me, own = lax.axis_index("rows"), lax.axis_index("owner")
    z, y, x = me // 8, (me // 4) % 2, me % 4
    peers = [((z + a) % 4) * 8 + ((y + b) % 2) * 4 + (x + c) % 4 for a, b, c in NEAREST]
    half = own // 2
    across = (own + 2) % 4
    beside = [
        (across, z * 8 + ((y + half) % 2) * 4 + x),
        (across, z * 8 + ((y + 1 - half) % 2) * 4 + x),
        (own + 1 - 2 * (own % 2), me),
    ]
    sources = ((w_gate, v_gate), (w_up, v_up))

    def arrival(m, p, k):
        return pltpu.make_async_copy(
            sources[m][k].at[pl.ds(2 * p, 2)],
            (w_in, v_in)[k].at[m, pl.ds(2 * p, 2)],
            in_sem.at[m, p, k],
        )

    barrier = pltpu.get_barrier_semaphore()
    for peer in reversed(peers):
        pl.semaphore_signal(barrier, inc=1, device_id=(own, peer), device_id_type=MESH)
    for other in beside:
        pl.semaphore_signal(barrier, inc=1, device_id=other, device_id_type=MESH)

    small = [
        pltpu.make_async_copy(a, b, small_sem.at[i])
        for i, (a, b) in enumerate(((mix_hbm, mix), (weight_hbm, weight), (gain_hbm, gain)))
    ]
    for copy in small:
        copy.start()
    for p in range(AHEAD):
        for k in range(2):
            arrival(0, p, k).start()

    for copy in small:
        copy.wait()

    def code(m, p, ahead):
        if ahead is not None:
            for k in range(2):
                arrival(ahead, (p + AHEAD) % 8, k).start()
        for k in range(2):
            arrival(m, p, k).wait()
        for q in range(8):
            cols = pl.ds(128 * q, 128)
            halves = []
            for h in range(2):
                e = 2 * p + h
                share = mix[e]
                f = share * w_in[m, e, :, cols] + (1.0 - share) * v_in[m, e, :, cols]
                size = jnp.abs(f)
                peak = jnp.max(size, axis=0, keepdims=True)
                peak = (peak * (1.0 + 2.0**-7)).astype(jnp.bfloat16).astype(jnp.float32)
                peaks[16 * m + e, :, cols] = peak
                rate = jnp.where(peak > 1e-30, SPAN / peak, 0.0)
                level = jnp.exp2(size * rate - LOW)
                halves.append(jnp.where(f < 0, -level, level))
            block = jnp.concatenate(halves, axis=0).T.astype(jnp.bfloat16)
            for r in range(4):
                sent[8 * m + p, 4 * q + r] = block[32 * r : 32 * r + 32]
        landed[8 * m + p, me] = sent[8 * m + p, me]

    def code_all(m, begin, end, ahead):
        def step(p, carry):
            code(m, p, ahead)
            return carry

        lax.fori_loop(begin, end, step, 0)

    def ship(c, carry):
        for peer in peers:
            pltpu.make_async_remote_copy(
                src_ref=sent.at[c, peer], dst_ref=landed.at[c, me],
                send_sem=send_sem.at[c], recv_sem=recv_sem.at[c],
                device_id=(own, peer), device_id_type=MESH,
            ).start()
        return carry

    code_all(0, 0, 4, 0)
    pl.semaphore_wait(barrier, 34)
    lax.fori_loop(0, FIRST, ship, 0)
    code_all(0, 4, 8, 1)
    code_all(1, 0, 4, 1)
    code_all(1, 4, 8, None)

    group = lax.broadcasted_iota(jnp.int32, (8, 128), 1) // 32
    routed = weight[...] * gain[...]
    routed = jnp.concatenate([routed[:8], routed[8:]], axis=1)
    for q in range(8):
        blocks = [peaks[8 * k : 8 * k + 8, 0, 128 * q : 128 * q + 128] for k in range(4)]
        for r in range(4):
            turned = blocks[r]
            for k in range(4):
                if k != r:
                    turned = jnp.where(
                        group == k, pltpu.roll(blocks[k], (32 * (k - r)) % 128, 1), turned
                    )
            sent_side[4 * q + r] = jnp.concatenate([turned, routed], axis=0).astype(jnp.bfloat16)
    landed_side[me] = sent_side[me]

    for peer in peers:
        pltpu.make_async_remote_copy(
            src_ref=sent_side.at[peer], dst_ref=landed_side.at[me],
            send_sem=side_send, recv_sem=side_recv,
            device_id=(own, peer), device_id_type=MESH,
        ).start()

    lax.fori_loop(FIRST, SECOND, ship, 0)

    def all_side():
        return pltpu.make_async_remote_copy(
            src_ref=sent_side.at[pl.ds(0, 31)], dst_ref=landed_side.at[pl.ds(0, 31)],
            send_sem=side_send, recv_sem=side_recv, device_id=(own, peers[0]), device_id_type=MESH,
        )

    def all_codes(c):
        return pltpu.make_async_remote_copy(
            src_ref=sent.at[c, pl.ds(0, 31)], dst_ref=landed.at[c, pl.ds(0, 31)],
            send_sem=send_sem.at[c], recv_sem=recv_sem.at[c],
            device_id=(own, peers[0]), device_id_type=MESH,
        )

    all_side().wait_recv()
    side[...] = landed_side[...].astype(jnp.float32)

    for k in range(16):
        for h, block in enumerate(swap_halves(side[2 * k, 8:, :], side[2 * k + 1, 8:, :])):
            lines[own, 8 * h : 8 * h + 8, 128 * k : 128 * k + 128] = block.astype(jnp.bfloat16)

    def pass_on(n, block, columns, to):
        return pltpu.make_async_remote_copy(
            src_ref=lines.at[block, :, columns], dst_ref=lines.at[block, :, columns],
            send_sem=line_send.at[n], recv_sem=line_recv.at[n],
            device_id=to, device_id_type=MESH,
        )

    whole = pl.ds(0, 2048)
    upward = pass_on(0, own, pl.ds(0, 1024), beside[0])
    downward = pass_on(1, own, pl.ds(1024, 1024), beside[1])
    over = pass_on(2, own, whole, beside[2])
    relay = pass_on(3, across, whole, beside[2])
    for copy in (upward, downward, over):
        copy.start()

    lax.fori_loop(SECOND, 16, ship, 0)

    at = lax.broadcasted_iota(jnp.int32, (32, 2048), 1) // 64
    picks = (at == lax.broadcasted_iota(jnp.int32, (32, 2048), 0)).astype(jnp.bfloat16)
    for r in range(8):
        turned = side[:, r, :].T.astype(jnp.bfloat16)
        spread[r] = jnp.dot(turned, picks, preferred_element_type=jnp.float32)

    scales[...] = jnp.zeros_like(scales)
    for m, out in enumerate((out_gate, out_up)):

        def decode(p, carry, m=m, out=out):
            c = 8 * m + p
            all_codes(c).wait_recv()
            rows = []
            for h in range(2):
                e = 2 * p + h
                rows.append((e % 8, pl.ds(pl.multiple_of(32 * (2 * m + e // 8), 32), 32)))
            sums = [jnp.zeros((32, 128), jnp.float32)] * 2
            for k in range(16):
                levels = []
                for s in range(2):
                    block = landed[c, 2 * k + s].astype(jnp.float32)
                    size = jnp.log2(jnp.abs(block)) + LOW
                    levels.append(jnp.where(block < 0, -size, size))
                for h, level in enumerate(swap_halves(*levels)):
                    f = level * spread[rows[h][0], rows[h][1], 128 * k : 128 * k + 128]
                    sums[h] += f * f
                    mixed[h, :, 128 * k : 128 * k + 128] = f
            lane = lax.broadcasted_iota(jnp.int32, (32, 128), 1)
            for h in range(2):
                e = 2 * p + h
                scale = jnp.sqrt(jnp.sum(sums[h], axis=1, keepdims=True))
                scales[...] = jnp.where(lane == 16 * m + e, scale * (1.0 / SPAN), scales[...])
                out[e] = (mixed[h] * (1.0 / scale)).astype(jnp.bfloat16)
            return carry

        if m == 0:
            lax.fori_loop(0, 8, decode, 0)
        else:
            lax.fori_loop(0, 5, decode, 0)
            upward.wait_recv()
            downward.wait_recv()
            relay.start()
            lax.fori_loop(5, 8, decode, 0)

    turned = scales[...].T
    out_scale_gate[...] = turned[:16]
    out_scale_up[...] = turned[16:32]

    over.wait()
    relay.wait()
    upward.wait_send()
    downward.wait_send()
    for o in range(4):
        out_router[16 * o : 16 * o + 16] = lines[o]

    all_side().wait_send()

    def drain(c, carry):
        all_codes(c).wait_send()
        return carry

    lax.fori_loop(0, 16, drain, 0)


def write_out(*refs):
    sems = refs[-1]
    n = (len(refs) - 1) // 2
    copies = [
        pltpu.make_async_copy(refs[i], refs[n + i], sems.at[i]) for i in range(n)
    ]
    for copy in copies:
        copy.start()
    for copy in copies:
        copy.wait()


def body(w_gate, avg_gate, w_up, avg_up, mix_share, router_weight, router_gain):
    vmem = pl.BlockSpec(memory_space=pltpu.VMEM)
    hbm = pl.BlockSpec(memory_space=pltpu.HBM)
    f32, bf16 = jnp.float32, jnp.bfloat16
    shapes = [
        ((16, 32, 2048), bf16),
        ((16, 32, 2048), bf16),
        ((16, 32), f32),
        ((16, 32), f32),
        ((64, 2048), bf16),
    ]
    results = pl.pallas_call(
        exchange,
        out_shape=[pltpu.VMEM(*shape) for shape in shapes],
        in_specs=[hbm] * 7,
        out_specs=[vmem] * 5,
        scratch_shapes=[
            pltpu.SMEM((16,), f32),
            pltpu.VMEM((16, 64), f32),
            pltpu.VMEM((1, 64), f32),
            pltpu.VMEM((2, 16, 64, 1024), f32),
            pltpu.VMEM((2, 16, 64, 1024), f32),
            pltpu.VMEM((32, 1, 1024), f32),
            pltpu.VMEM((16, 32, 32, 128), bf16),
            pltpu.VMEM((16, 32, 32, 128), bf16),
            pltpu.VMEM((32, 16, 128), bf16),
            pltpu.VMEM((32, 16, 128), bf16),
            pltpu.VMEM((32, 16, 128), f32),
            pltpu.VMEM((8, 128, 2048), f32),
            pltpu.VMEM((2, 32, 2048), f32),
            pltpu.VMEM((4, 16, 2048), bf16),
            pltpu.VMEM((32, 128), f32),
            pltpu.SemaphoreType.DMA((3,)),
            pltpu.SemaphoreType.DMA((2, 8, 2)),
            pltpu.SemaphoreType.DMA((16,)),
            pltpu.SemaphoreType.DMA((16,)),
            pltpu.SemaphoreType.DMA,
            pltpu.SemaphoreType.DMA,
            pltpu.SemaphoreType.DMA((4,)),
            pltpu.SemaphoreType.DMA((4,)),
        ],
        compiler_params=pltpu.CompilerParams(
            collective_id=0, has_side_effects=True, vmem_limit_bytes=40 << 20
        ),
        name="exchange",
    )(
        *[
            pltpu.with_memory_space_constraint(a, pltpu.HBM)
            for a in (
                mix_share, w_gate, avg_gate, w_up, avg_up,
                router_weight.T, router_gain.reshape(1, 64),
            )
        ]
    )
    serve_gate, serve_up, scale_gate, scale_up, router = pl.pallas_call(
        write_out,
        out_shape=[jax.ShapeDtypeStruct(*shape) for shape in shapes],
        in_specs=[vmem] * 5,
        out_specs=[hbm] * 5,
        scratch_shapes=[pltpu.SemaphoreType.DMA((5,))],
        compiler_params=pltpu.CompilerParams(vmem_limit_bytes=4 << 20),
        name="write_out",
    )(*[pltpu.with_memory_space_constraint(a, pltpu.VMEM) for a in results])
    return (
        jnp.swapaxes(serve_gate, 1, 2),
        jnp.swapaxes(serve_up, 1, 2),
        scale_gate,
        scale_up,
        router.T,
    )


def solution(mesh):
    return jax.shard_map(
        body,
        mesh=mesh,
        in_specs=(
            P("owner", "rows", None),
            P("owner", "rows", None),
            P("owner", "rows", None),
            P("owner", "rows", None),
            P("owner"),
            P("rows", "owner"),
            P("rows"),
        ),
        out_specs=(
            P("owner", None, "rows"),
            P("owner", None, "rows"),
            P("owner", "rows"),
            P("owner", "rows"),
            P(),
        ),
        check_vma=False,
    )
```

```python
import functools

import jax
import jax.numpy as jnp
from jax import lax
from jax.experimental import pallas as pl
from jax.experimental.pallas import tpu as pltpu
from jax.sharding import PartitionSpec as P

MESH = pl.DeviceIdType.MESH
SPAN = 252.0
LOW = 125.0
AHEAD = 4
FIRST = 4
SECOND = 12
OFFSETS = [(a, b, c) for a in range(4) for b in range(2) for c in range(4)][1:]
NEAREST = sorted(OFFSETS, key=lambda o: min(o[0], 4 - o[0]) + 2 * o[1] + min(o[2], 4 - o[2]))


def left_half(shape):
    return lax.broadcasted_iota(jnp.int32, shape, len(shape) - 1) < 64


def swap_halves(a, b):
    left = left_half(a.shape)
    return jnp.where(left, a, pltpu.roll(b, 64, 1)), jnp.where(left, pltpu.roll(a, 64, 1), b)


def exchange(
    mix_hbm, w_gate, v_gate, w_up, v_up, weight_hbm, gain_hbm,
    out_gate, out_up, out_scale_gate, out_scale_up, out_router,
    mix, weight, gain, w_in, v_in, peaks, sent, landed, sent_side, landed_side, side, spread, mixed, lines, scales,
    small_sem, in_sem, send_sem, recv_sem, side_send, side_recv, line_send, line_recv,
):
    me, own = lax.axis_index("rows"), lax.axis_index("owner")
    z, y, x = me // 8, (me // 4) % 2, me % 4
    peers = [((z + a) % 4) * 8 + ((y + b) % 2) * 4 + (x + c) % 4 for a, b, c in NEAREST]
    half = own // 2
    across = (own + 2) % 4
    beside = [
        (across, z * 8 + ((y + half) % 2) * 4 + x),
        (across, z * 8 + ((y + 1 - half) % 2) * 4 + x),
        (own + 1 - 2 * (own % 2), me),
    ]
    sources = ((w_gate, v_gate), (w_up, v_up))

    def arrival(m, p, k):
        return pltpu.make_async_copy(
            sources[m][k].at[pl.ds(2 * p, 2)],
            (w_in, v_in)[k].at[m, pl.ds(2 * p, 2)],
            in_sem.at[m, p, k],
        )

    barrier = pltpu.get_barrier_semaphore()
    for peer in reversed(peers):
        pl.semaphore_signal(barrier, inc=1, device_id=(own, peer), device_id_type=MESH)
    for other in beside:
        pl.semaphore_signal(barrier, inc=1, device_id=other, device_id_type=MESH)

    small = [
        pltpu.make_async_copy(a, b, small_sem.at[i])
        for i, (a, b) in enumerate(((mix_hbm, mix), (weight_hbm, weight), (gain_hbm, gain)))
    ]
    small[0].start()
    for p in range(AHEAD):
        for k in range(2):
            arrival(0, p, k).start()
    for copy in small[1:]:
        copy.start()

    small[0].wait()

    def code(m, p, ahead):
        if ahead is not None:
            for k in range(2):
                arrival(ahead, (p + AHEAD) % 8, k).start()
        for k in range(2):
            arrival(m, p, k).wait()
        for q in range(8):
            cols = pl.ds(128 * q, 128)
            halves = []
            for h in range(2):
                e = 2 * p + h
                share = mix[e]
                f = share * w_in[m, e, :, cols] + (1.0 - share) * v_in[m, e, :, cols]
                size = jnp.abs(f)
                peak = jnp.max(size, axis=0, keepdims=True)
                peak = (peak * (1.0 + 2.0**-7)).astype(jnp.bfloat16).astype(jnp.float32)
                peaks[16 * m + e, :, cols] = peak
                rate = jnp.where(peak > 1e-30, SPAN / peak, 0.0)
                level = jnp.exp2(size * rate - LOW)
                halves.append(jnp.where(f < 0, -level, level))
            block = jnp.concatenate(halves, axis=0).T.astype(jnp.bfloat16)
            for r in range(4):
                sent[8 * m + p, 4 * q + r] = block[32 * r : 32 * r + 32]
        landed[8 * m + p, me] = sent[8 * m + p, me]

    def code_all(m, begin, end, ahead):
        def step(p, carry):
            code(m, p, ahead)
            return carry

        lax.fori_loop(begin, end, step, 0)

    def ship(c, carry):
        for peer in peers:
            pltpu.make_async_remote_copy(
                src_ref=sent.at[c, peer], dst_ref=landed.at[c, me],
                send_sem=send_sem.at[c], recv_sem=recv_sem.at[c],
                device_id=(own, peer), device_id_type=MESH,
            ).start()
        return carry

    code_all(0, 0, 1, 0)
    pl.semaphore_wait(barrier, 34)
    ship(0, 0)

    def code_and_ship(p, carry):
        code(0, p, 0)
        return ship(p, carry)

    lax.fori_loop(1, FIRST, code_and_ship, 0)
    code_all(0, 4, 8, 1)
    code_all(1, 0, 4, 1)
    code_all(1, 4, 8, None)

    group = lax.broadcasted_iota(jnp.int32, (8, 128), 1) // 32
    for copy in small[1:]:
        copy.wait()
    routed = weight[...] * gain[...]
    routed = jnp.concatenate([routed[:8], routed[8:]], axis=1)
    for q in range(8):
        blocks = [peaks[8 * k : 8 * k + 8, 0, 128 * q : 128 * q + 128] for k in range(4)]
        for r in range(4):
            turned = blocks[r]
            for k in range(4):
                if k != r:
                    turned = jnp.where(
                        group == k, pltpu.roll(blocks[k], (32 * (k - r)) % 128, 1), turned
                    )
            sent_side[4 * q + r] = jnp.concatenate([turned, routed], axis=0).astype(jnp.bfloat16)
    landed_side[me] = sent_side[me]

    for peer in peers:
        pltpu.make_async_remote_copy(
            src_ref=sent_side.at[peer], dst_ref=landed_side.at[me],
            send_sem=side_send, recv_sem=side_recv,
            device_id=(own, peer), device_id_type=MESH,
        ).start()

    lax.fori_loop(FIRST, SECOND, ship, 0)

    def all_side():
        return pltpu.make_async_remote_copy(
            src_ref=sent_side.at[pl.ds(0, 31)], dst_ref=landed_side.at[pl.ds(0, 31)],
            send_sem=side_send, recv_sem=side_recv, device_id=(own, peers[0]), device_id_type=MESH,
        )

    def all_codes(c):
        return pltpu.make_async_remote_copy(
            src_ref=sent.at[c, pl.ds(0, 31)], dst_ref=landed.at[c, pl.ds(0, 31)],
            send_sem=send_sem.at[c], recv_sem=recv_sem.at[c],
            device_id=(own, peers[0]), device_id_type=MESH,
        )

    all_side().wait_recv()
    side[...] = landed_side[...].astype(jnp.float32)

    for k in range(16):
        for h, block in enumerate(swap_halves(side[2 * k, 8:, :], side[2 * k + 1, 8:, :])):
            lines[own, 8 * h : 8 * h + 8, 128 * k : 128 * k + 128] = block.astype(jnp.bfloat16)

    def pass_on(n, block, columns, to):
        return pltpu.make_async_remote_copy(
            src_ref=lines.at[block, :, columns], dst_ref=lines.at[block, :, columns],
            send_sem=line_send.at[n], recv_sem=line_recv.at[n],
            device_id=to, device_id_type=MESH,
        )

    whole = pl.ds(0, 2048)
    upward = pass_on(0, own, pl.ds(0, 1024), beside[0])
    downward = pass_on(1, own, pl.ds(1024, 1024), beside[1])
    over = pass_on(2, own, whole, beside[2])
    relay = pass_on(3, across, whole, beside[2])
    for copy in (upward, downward, over):
        copy.start()

    lax.fori_loop(SECOND, 16, ship, 0)

    at = lax.broadcasted_iota(jnp.int32, (32, 2048), 1) // 64
    picks = (at == lax.broadcasted_iota(jnp.int32, (32, 2048), 0)).astype(jnp.bfloat16)
    for r in range(8):
        turned = side[:, r, :].T.astype(jnp.bfloat16)
        spread[r] = jnp.dot(turned, picks, preferred_element_type=jnp.float32)

    scales[...] = jnp.zeros_like(scales)
    for m, out in enumerate((out_gate, out_up)):

        def decode(p, carry, m=m, out=out):
            c = 8 * m + p
            all_codes(c).wait_recv()
            rows = []
            for h in range(2):
                e = 2 * p + h
                rows.append((e % 8, pl.ds(pl.multiple_of(32 * (2 * m + e // 8), 32), 32)))
            sums = [jnp.zeros((32, 128), jnp.float32)] * 2
            for k in range(16):
                levels = []
                for s in range(2):
                    block = landed[c, 2 * k + s].astype(jnp.float32)
                    size = jnp.log2(jnp.abs(block)) + LOW
                    levels.append(jnp.where(block < 0, -size, size))
                for h, level in enumerate(swap_halves(*levels)):
                    f = level * spread[rows[h][0], rows[h][1], 128 * k : 128 * k + 128]
                    sums[h] += f * f
                    mixed[h, :, 128 * k : 128 * k + 128] = f
            lane = lax.broadcasted_iota(jnp.int32, (32, 128), 1)
            for h in range(2):
                e = 2 * p + h
                scale = jnp.sqrt(jnp.sum(sums[h], axis=1, keepdims=True))
                scales[...] = jnp.where(lane == 16 * m + e, scale * (1.0 / SPAN), scales[...])
                out[e] = (mixed[h] * (1.0 / scale)).astype(jnp.bfloat16)
            return carry

        if m == 0:
            lax.fori_loop(0, 8, decode, 0)
        else:
            lax.fori_loop(0, 5, decode, 0)
            upward.wait_recv()
            downward.wait_recv()
            relay.start()
            lax.fori_loop(5, 8, decode, 0)

    turned = scales[...].T
    out_scale_gate[...] = turned[:16]
    out_scale_up[...] = turned[16:32]

    over.wait()
    relay.wait()
    upward.wait_send()
    downward.wait_send()
    for o in range(4):
        out_router[16 * o : 16 * o + 16] = lines[o]

    all_side().wait_send()

    def drain(c, carry):
        all_codes(c).wait_send()
        return carry

    lax.fori_loop(0, 16, drain, 0)


def write_out(*refs):
    sems = refs[-1]
    n = (len(refs) - 1) // 2
    copies = [
        pltpu.make_async_copy(refs[i], refs[n + i], sems.at[i]) for i in range(n)
    ]
    for copy in copies:
        copy.start()
    for copy in copies:
        copy.wait()


def body(w_gate, avg_gate, w_up, avg_up, mix_share, router_weight, router_gain):
    vmem = pl.BlockSpec(memory_space=pltpu.VMEM)
    hbm = pl.BlockSpec(memory_space=pltpu.HBM)
    f32, bf16 = jnp.float32, jnp.bfloat16
    shapes = [
        ((16, 32, 2048), bf16),
        ((16, 32, 2048), bf16),
        ((16, 32), f32),
        ((16, 32), f32),
        ((64, 2048), bf16),
    ]
    results = pl.pallas_call(
        exchange,
        out_shape=[pltpu.VMEM(*shape) for shape in shapes],
        in_specs=[hbm] * 7,
        out_specs=[vmem] * 5,
        scratch_shapes=[
            pltpu.SMEM((16,), f32),
            pltpu.VMEM((16, 64), f32),
            pltpu.VMEM((1, 64), f32),
            pltpu.VMEM((2, 16, 64, 1024), f32),
            pltpu.VMEM((2, 16, 64, 1024), f32),
            pltpu.VMEM((32, 1, 1024), f32),
            pltpu.VMEM((16, 32, 32, 128), bf16),
            pltpu.VMEM((16, 32, 32, 128), bf16),
            pltpu.VMEM((32, 16, 128), bf16),
            pltpu.VMEM((32, 16, 128), bf16),
            pltpu.VMEM((32, 16, 128), f32),
            pltpu.VMEM((8, 128, 2048), f32),
            pltpu.VMEM((2, 32, 2048), f32),
            pltpu.VMEM((4, 16, 2048), bf16),
            pltpu.VMEM((32, 128), f32),
            pltpu.SemaphoreType.DMA((3,)),
            pltpu.SemaphoreType.DMA((2, 8, 2)),
            pltpu.SemaphoreType.DMA((16,)),
            pltpu.SemaphoreType.DMA((16,)),
            pltpu.SemaphoreType.DMA,
            pltpu.SemaphoreType.DMA,
            pltpu.SemaphoreType.DMA((4,)),
            pltpu.SemaphoreType.DMA((4,)),
        ],
        compiler_params=pltpu.CompilerParams(
            collective_id=0, has_side_effects=True, vmem_limit_bytes=40 << 20
        ),
        name="exchange",
    )(
        *[
            pltpu.with_memory_space_constraint(a, pltpu.HBM)
            for a in (
                mix_share, w_gate, avg_gate, w_up, avg_up,
                router_weight.T, router_gain.reshape(1, 64),
            )
        ]
    )
    serve_gate, serve_up, scale_gate, scale_up, router = pl.pallas_call(
        write_out,
        out_shape=[jax.ShapeDtypeStruct(*shape) for shape in shapes],
        in_specs=[vmem] * 5,
        out_specs=[hbm] * 5,
        scratch_shapes=[pltpu.SemaphoreType.DMA((5,))],
        compiler_params=pltpu.CompilerParams(vmem_limit_bytes=4 << 20),
        name="write_out",
    )(*[pltpu.with_memory_space_constraint(a, pltpu.VMEM) for a in results])
    return (
        jnp.swapaxes(serve_gate, 1, 2),
        jnp.swapaxes(serve_up, 1, 2),
        scale_gate,
        scale_up,
        router.T,
    )


def solution(mesh):
    return jax.shard_map(
        body,
        mesh=mesh,
        in_specs=(
            P("owner", "rows", None),
            P("owner", "rows", None),
            P("owner", "rows", None),
            P("owner", "rows", None),
            P("owner"),
            P("rows", "owner"),
            P("rows"),
        ),
        out_specs=(
            P("owner", None, "rows"),
            P("owner", None, "rows"),
            P("owner", "rows"),
            P("owner", "rows"),
            P(),
        ),
        check_vma=False,
    )
```

```python
import functools

import jax
import jax.numpy as jnp
from jax import lax
from jax.experimental import pallas as pl
from jax.experimental.pallas import tpu as pltpu
from jax.sharding import PartitionSpec as P

MESH = pl.DeviceIdType.MESH
SPAN = 252.0
LOW = 125.0
AHEAD = 4
FIRST = 4
SECOND = 12
OFFSETS = [(a, b, c) for a in range(4) for b in range(2) for c in range(4)][1:]
FARTHEST = sorted(OFFSETS, key=lambda o: -min(o[0], 4 - o[0]) - 2 * o[1] - min(o[2], 4 - o[2]))


def left_half(shape):
    return lax.broadcasted_iota(jnp.int32, shape, len(shape) - 1) < 64


def swap_halves(a, b):
    left = left_half(a.shape)
    return jnp.where(left, a, pltpu.roll(b, 64, 1)), jnp.where(left, pltpu.roll(a, 64, 1), b)


def exchange(
    mix_hbm, w_gate, v_gate, w_up, v_up, weight_hbm, gain_hbm,
    out_gate, out_up, out_scale_gate, out_scale_up, out_router,
    mix, weight, gain, w_in, v_in, peaks, sent, landed, sent_side, landed_side, side, spread, mixed, lines, scales,
    small_sem, in_sem, send_sem, recv_sem, side_send, side_recv, line_send, line_recv,
):
    me, own = lax.axis_index("rows"), lax.axis_index("owner")
    z, y, x = lax.div(me, 8), lax.rem(lax.div(me, 4), 2), lax.rem(me, 4)
    zs = [lax.rem(z + a, 4) * 8 for a in range(4)]
    ys = [y * 4, (1 - y) * 4]
    xs = [lax.rem(x + c, 4) for c in range(4)]
    peers = [zs[a] + ys[b] + xs[c] for a, b, c in FARTHEST]
    half = lax.div(own, 2)
    across = lax.rem(own + 2, 4)
    beside = [
        (across, z * 8 + lax.rem(y + half, 2) * 4 + x),
        (across, z * 8 + lax.rem(y + 1 - half, 2) * 4 + x),
        (own + 1 - 2 * lax.rem(own, 2), me),
    ]
    sources = ((w_gate, v_gate), (w_up, v_up))

    def arrival(m, p, k):
        return pltpu.make_async_copy(
            sources[m][k].at[pl.ds(2 * p, 2)],
            (w_in, v_in)[k].at[m, pl.ds(2 * p, 2)],
            in_sem.at[(p % AHEAD) if isinstance(p, int) else lax.rem(p, AHEAD), k],
        )

    barrier = pltpu.get_barrier_semaphore()
    for peer in peers:
        pl.semaphore_signal(barrier, inc=1, device_id=(own, peer), device_id_type=MESH)
    for other in beside:
        pl.semaphore_signal(barrier, inc=1, device_id=other, device_id_type=MESH)

    small = [
        pltpu.make_async_copy(a, b, small_sem.at[i])
        for i, (a, b) in enumerate(((mix_hbm, mix), (weight_hbm, weight), (gain_hbm, gain)))
    ]
    small[0].start()
    for p in range(AHEAD):
        for k in range(2):
            arrival(0, p, k).start()
    for copy in small[1:]:
        copy.start()

    small[0].wait()

    def code(m, p, ahead):
        for k in range(2):
            arrival(m, p, k).wait()
        if ahead is not None:
            for k in range(2):
                arrival(ahead, lax.rem(p + AHEAD, 8), k).start()
        for q in range(8):
            cols = pl.ds(128 * q, 128)
            halves = []
            for h in range(2):
                e = 2 * p + h
                share = mix[e]
                f = share * w_in[m, e, :, cols] + (1.0 - share) * v_in[m, e, :, cols]
                size = jnp.abs(f)
                peak = jnp.max(size, axis=0, keepdims=True)
                peak = (peak * (1.0 + 2.0**-7)).astype(jnp.bfloat16).astype(jnp.float32)
                peaks[16 * m + e, :, cols] = peak
                rate = jnp.where(peak > 1e-30, SPAN / peak, 0.0)
                level = jnp.exp2(size * rate - LOW)
                halves.append(jnp.where(f < 0, -level, level))
            block = jnp.concatenate(halves, axis=0).T.astype(jnp.bfloat16)
            for r in range(4):
                sent[8 * m + p, 4 * q + r] = block[32 * r : 32 * r + 32]
        landed[8 * m + p, me] = sent[8 * m + p, me]

    def code_all(m, begin, end, ahead):
        def step(p, carry):
            code(m, p, ahead)
            return carry

        lax.fori_loop(begin, end, step, 0)

    def ship(c, carry):
        for peer in peers:
            pltpu.make_async_remote_copy(
                src_ref=sent.at[c, peer], dst_ref=landed.at[c, me],
                send_sem=send_sem, recv_sem=recv_sem.at[c],
                device_id=(own, peer), device_id_type=MESH,
            ).start()
        return carry

    code_all(0, 0, 1, 0)
    pl.semaphore_wait(barrier, 34)
    ship(0, 0)

    def code_and_ship(p, carry):
        code(0, p, 0)
        return ship(p, carry)

    lax.fori_loop(1, FIRST, code_and_ship, 0)
    code_all(0, 4, 8, 1)
    code_all(1, 0, 4, 1)
    code_all(1, 4, 8, None)

    group = lax.broadcasted_iota(jnp.int32, (8, 128), 1) // 32
    for copy in small[1:]:
        copy.wait()
    routed = weight[...] * gain[...]
    routed = jnp.concatenate([routed[:8], routed[8:]], axis=1)
    for q in range(8):
        blocks = [peaks[8 * k : 8 * k + 8, 0, 128 * q : 128 * q + 128] for k in range(4)]
        for r in range(4):
            turned = blocks[r]
            for k in range(4):
                if k != r:
                    turned = jnp.where(
                        group == k, pltpu.roll(blocks[k], (32 * (k - r)) % 128, 1), turned
                    )
            sent_side[4 * q + r] = jnp.concatenate([turned, routed], axis=0).astype(jnp.bfloat16)
    landed_side[me] = sent_side[me]

    for peer in peers:
        pltpu.make_async_remote_copy(
            src_ref=sent_side.at[peer], dst_ref=landed_side.at[me],
            send_sem=side_send, recv_sem=side_recv,
            device_id=(own, peer), device_id_type=MESH,
        ).start()

    lax.fori_loop(FIRST, SECOND, ship, 0)

    def all_side():
        return pltpu.make_async_remote_copy(
            src_ref=sent_side.at[pl.ds(0, 31)], dst_ref=landed_side.at[pl.ds(0, 31)],
            send_sem=side_send, recv_sem=side_recv, device_id=(own, peers[0]), device_id_type=MESH,
        )

    def all_codes(c):
        return pltpu.make_async_remote_copy(
            src_ref=sent.at[c, pl.ds(0, 31)], dst_ref=landed.at[c, pl.ds(0, 31)],
            send_sem=send_sem, recv_sem=recv_sem.at[c],
            device_id=(own, peers[0]), device_id_type=MESH,
        )

    all_side().wait_recv()
    side[...] = landed_side[...].astype(jnp.float32)

    for k in range(16):
        for h, block in enumerate(swap_halves(side[2 * k, 8:, :], side[2 * k + 1, 8:, :])):
            lines[own, 8 * h : 8 * h + 8, 128 * k : 128 * k + 128] = block.astype(jnp.bfloat16)

    def pass_on(n, block, columns, to):
        return pltpu.make_async_remote_copy(
            src_ref=lines.at[block, :, columns], dst_ref=lines.at[block, :, columns],
            send_sem=line_send.at[n], recv_sem=line_recv.at[n],
            device_id=to, device_id_type=MESH,
        )

    whole = pl.ds(0, 2048)
    upward = pass_on(0, own, pl.ds(0, 1024), beside[0])
    downward = pass_on(1, own, pl.ds(1024, 1024), beside[1])
    over = pass_on(2, own, whole, beside[2])
    relay = pass_on(3, across, whole, beside[2])
    for copy in (upward, downward, over):
        copy.start()

    lax.fori_loop(SECOND, 16, ship, 0)

    at = lax.broadcasted_iota(jnp.int32, (32, 2048), 1) // 64
    picks = (at == lax.broadcasted_iota(jnp.int32, (32, 2048), 0)).astype(jnp.bfloat16)
    for r in range(8):
        turned = side[:, r, :].T.astype(jnp.bfloat16)
        spread[r] = jnp.dot(turned, picks, preferred_element_type=jnp.float32)

    scales[...] = jnp.zeros_like(scales)
    for m, out in enumerate((out_gate, out_up)):

        def decode(p, carry, m=m, out=out):
            c = 8 * m + p
            all_codes(c).wait_recv()
            rows = []
            for h in range(2):
                e = 2 * p + h
                rows.append((e % 8, pl.ds(pl.multiple_of(32 * (2 * m + e // 8), 32), 32)))
            sums = [jnp.zeros((32, 128), jnp.float32)] * 2
            for k in range(16):
                levels = []
                for s in range(2):
                    block = landed[c, 2 * k + s].astype(jnp.float32)
                    size = jnp.log2(jnp.abs(block)) + LOW
                    levels.append(jnp.where(block < 0, -size, size))
                for h, level in enumerate(swap_halves(*levels)):
                    f = level * spread[rows[h][0], rows[h][1], 128 * k : 128 * k + 128]
                    sums[h] += f * f
                    mixed[h, :, 128 * k : 128 * k + 128] = f
            lane = lax.broadcasted_iota(jnp.int32, (32, 128), 1)
            for h in range(2):
                e = 2 * p + h
                scale = jnp.sqrt(jnp.sum(sums[h], axis=1, keepdims=True))
                scales[...] = jnp.where(lane == 16 * m + e, scale * (1.0 / SPAN), scales[...])
                out[e] = (mixed[h] * (1.0 / scale)).astype(jnp.bfloat16)
            return carry

        if m == 0:
            lax.fori_loop(0, 8, decode, 0)
        else:
            lax.fori_loop(0, 5, decode, 0)
            upward.wait_recv()
            downward.wait_recv()
            relay.start()
            lax.fori_loop(5, 8, decode, 0)

    turned = scales[...].T
    out_scale_gate[...] = turned[:16]
    out_scale_up[...] = turned[16:32]

    over.wait()
    relay.wait()
    upward.wait_send()
    downward.wait_send()
    for o in range(4):
        out_router[16 * o : 16 * o + 16] = lines[o]

    all_side().wait_send()

    pltpu.make_async_remote_copy(
        src_ref=sent.at[:, pl.ds(0, 31)], dst_ref=landed.at[:, pl.ds(0, 31)],
        send_sem=send_sem, recv_sem=recv_sem.at[0],
        device_id=(own, peers[0]), device_id_type=MESH,
    ).wait_send()


def write_out(*refs):
    sems = refs[-1]
    n = (len(refs) - 1) // 2
    copies = [
        pltpu.make_async_copy(refs[i], refs[n + i], sems.at[i]) for i in range(n)
    ]
    for copy in copies:
        copy.start()
    for copy in copies:
        copy.wait()


def body(w_gate, avg_gate, w_up, avg_up, mix_share, router_weight, router_gain):
    vmem = pl.BlockSpec(memory_space=pltpu.VMEM)
    hbm = pl.BlockSpec(memory_space=pltpu.HBM)
    f32, bf16 = jnp.float32, jnp.bfloat16
    shapes = [
        ((16, 32, 2048), bf16),
        ((16, 32, 2048), bf16),
        ((16, 32), f32),
        ((16, 32), f32),
        ((64, 2048), bf16),
    ]
    results = pl.pallas_call(
        exchange,
        out_shape=[pltpu.VMEM(*shape) for shape in shapes],
        in_specs=[hbm] * 7,
        out_specs=[vmem] * 5,
        scratch_shapes=[
            pltpu.SMEM((16,), f32),
            pltpu.VMEM((16, 64), f32),
            pltpu.VMEM((1, 64), f32),
            pltpu.VMEM((2, 16, 64, 1024), f32),
            pltpu.VMEM((2, 16, 64, 1024), f32),
            pltpu.VMEM((32, 1, 1024), f32),
            pltpu.VMEM((16, 32, 32, 128), bf16),
            pltpu.VMEM((16, 32, 32, 128), bf16),
            pltpu.VMEM((32, 16, 128), bf16),
            pltpu.VMEM((32, 16, 128), bf16),
            pltpu.VMEM((32, 16, 128), f32),
            pltpu.VMEM((8, 128, 2048), f32),
            pltpu.VMEM((2, 32, 2048), f32),
            pltpu.VMEM((4, 16, 2048), bf16),
            pltpu.VMEM((32, 128), f32),
            pltpu.SemaphoreType.DMA((3,)),
            pltpu.SemaphoreType.DMA((AHEAD, 2)),
            pltpu.SemaphoreType.DMA,
            pltpu.SemaphoreType.DMA((16,)),
            pltpu.SemaphoreType.DMA,
            pltpu.SemaphoreType.DMA,
            pltpu.SemaphoreType.DMA((4,)),
            pltpu.SemaphoreType.DMA((4,)),
        ],
        compiler_params=pltpu.CompilerParams(
            collective_id=0, has_side_effects=True, vmem_limit_bytes=40 << 20
        ),
        name="exchange",
    )(
        *[
            pltpu.with_memory_space_constraint(a, pltpu.HBM)
            for a in (
                mix_share, w_gate, avg_gate, w_up, avg_up,
                router_weight.T, router_gain.reshape(1, 64),
            )
        ]
    )
    serve_gate, serve_up, scale_gate, scale_up, router = pl.pallas_call(
        write_out,
        out_shape=[jax.ShapeDtypeStruct(*shape) for shape in shapes],
        in_specs=[vmem] * 5,
        out_specs=[hbm] * 5,
        scratch_shapes=[pltpu.SemaphoreType.DMA((5,))],
        compiler_params=pltpu.CompilerParams(vmem_limit_bytes=4 << 20),
        name="write_out",
    )(*[pltpu.with_memory_space_constraint(a, pltpu.VMEM) for a in results])
    return (
        jnp.swapaxes(serve_gate, 1, 2),
        jnp.swapaxes(serve_up, 1, 2),
        scale_gate,
        scale_up,
        router.T,
    )


def solution(mesh):
    return jax.shard_map(
        body,
        mesh=mesh,
        in_specs=(
            P("owner", "rows", None),
            P("owner", "rows", None),
            P("owner", "rows", None),
            P("owner", "rows", None),
            P("owner"),
            P("rows", "owner"),
            P("rows"),
        ),
        out_specs=(
            P("owner", None, "rows"),
            P("owner", None, "rows"),
            P("owner", "rows"),
            P("owner", "rows"),
            P(),
        ),
        check_vma=False,
    )
```

```python
import functools

import jax
import jax.numpy as jnp
from jax import lax
from jax.experimental import pallas as pl
from jax.experimental.pallas import tpu as pltpu
from jax.sharding import PartitionSpec as P

MESH = pl.DeviceIdType.MESH
SPAN = 252.0
LOW = 125.0
AHEAD = 4
FIRST = 4
SECOND = 8
THIRD = 12
OFFSETS = [(a, b, c) for a in range(4) for b in range(2) for c in range(4)][1:]
FARTHEST = sorted(OFFSETS, key=lambda o: -min(o[0], 4 - o[0]) - 2 * o[1] - min(o[2], 4 - o[2]))


def left_half(shape):
    return lax.broadcasted_iota(jnp.int32, shape, len(shape) - 1) < 64


def swap_halves(a, b):
    left = left_half(a.shape)
    return jnp.where(left, a, pltpu.roll(b, 64, 1)), jnp.where(left, pltpu.roll(a, 64, 1), b)


def exchange(
    mix_hbm, w_gate, v_gate, w_up, v_up, weight_hbm, gain_hbm,
    out_gate, out_up, out_scale_gate, out_scale_up, out_router,
    mix, weight, gain, w_in, v_in, peaks, sent, landed, sent_side, landed_side, side, spread, mixed, gathered, lines, scales,
    small_sem, in_sem, send_sem, recv_sem, side_send, side_recv, gather_send, gather_recv, line_send, line_recv,
):
    me, own = lax.axis_index("rows"), lax.axis_index("owner")
    z, y, x = lax.div(me, 8), lax.rem(lax.div(me, 4), 2), lax.rem(me, 4)
    zs = [lax.rem(z + a, 4) * 8 for a in range(4)]
    ys = [y * 4, (1 - y) * 4]
    xs = [lax.rem(x + c, 4) for c in range(4)]
    peers = [zs[a] + ys[b] + xs[c] for a, b, c in FARTHEST]
    half = lax.div(own, 2)
    across = lax.rem(own + 2, 4)
    beside = [
        (across, z * 8 + lax.rem(y + half, 2) * 4 + x),
        (across, z * 8 + lax.rem(y + 1 - half, 2) * 4 + x),
        (own + 1 - 2 * lax.rem(own, 2), me),
    ]
    sources = ((w_gate, v_gate), (w_up, v_up))

    def arrival(m, p, k):
        return pltpu.make_async_copy(
            sources[m][k].at[pl.ds(2 * p, 2)],
            (w_in, v_in)[k].at[m, pl.ds(2 * p, 2)],
            in_sem.at[(p % AHEAD) if isinstance(p, int) else lax.rem(p, AHEAD), k],
        )

    barrier = pltpu.get_barrier_semaphore()
    for peer in peers:
        pl.semaphore_signal(barrier, inc=1, device_id=(own, peer), device_id_type=MESH)
    for other in beside:
        pl.semaphore_signal(barrier, inc=1, device_id=other, device_id_type=MESH)

    small = [
        pltpu.make_async_copy(a, b, small_sem.at[i])
        for i, (a, b) in enumerate(((mix_hbm, mix), (weight_hbm, weight), (gain_hbm, gain)))
    ]
    small[0].start()
    for p in range(AHEAD):
        for k in range(2):
            arrival(0, p, k).start()
    for copy in small[1:]:
        copy.start()

    small[0].wait()

    def code(m, p, ahead):
        for k in range(2):
            arrival(m, p, k).wait()
        if ahead is not None:
            for k in range(2):
                arrival(ahead, lax.rem(p + AHEAD, 8), k).start()
        for q in range(8):
            cols = pl.ds(128 * q, 128)
            halves = []
            for h in range(2):
                e = 2 * p + h
                share = mix[e]
                f = share * w_in[m, e, :, cols] + (1.0 - share) * v_in[m, e, :, cols]
                size = jnp.abs(f)
                peak = jnp.max(size, axis=0, keepdims=True)
                peak = (peak * (1.0 + 2.0**-7)).astype(jnp.bfloat16).astype(jnp.float32)
                peaks[16 * m + e, :, cols] = peak
                rate = jnp.where(peak > 1e-30, SPAN / peak, 0.0)
                level = jnp.exp2(size * rate - LOW)
                halves.append(jnp.where(f < 0, -level, level))
            block = jnp.concatenate(halves, axis=0).T.astype(jnp.bfloat16)
            for r in range(4):
                sent[8 * m + p, 4 * q + r] = block[32 * r : 32 * r + 32]
        landed[8 * m + p, me] = sent[8 * m + p, me]

    def code_all(m, begin, end, ahead):
        def step(p, carry):
            code(m, p, ahead)
            return carry

        lax.fori_loop(begin, end, step, 0)

    def gather(n, part, to):
        return pltpu.make_async_remote_copy(
            src_ref=part, dst_ref=part, send_sem=gather_send.at[n], recv_sem=gather_recv.at[n],
            device_id=(own, to), device_id_type=MESH,
        )

    along_y = gather(0, gathered.at[z, x, y], zs[0] + ys[1] + x)
    along_x = [gather(1, gathered.at[z, x], zs[0] + ys[0] + xs[c]) for c in (2, 1, 3)]
    along_z = [gather(2, gathered.at[z], zs[a] + ys[0] + x) for a in (2, 1, 3)]
    all_x = gather(1, gathered.at[0, pl.ds(0, 3)], peers[0])
    all_z = gather(2, gathered.at[pl.ds(0, 3)], peers[0])

    def ship(c, carry):
        for peer in peers:
            pltpu.make_async_remote_copy(
                src_ref=sent.at[c, peer], dst_ref=landed.at[c, me],
                send_sem=send_sem, recv_sem=recv_sem.at[c],
                device_id=(own, peer), device_id_type=MESH,
            ).start()
        return carry

    code_all(0, 0, 1, 0)
    for copy in small[1:]:
        copy.wait()
    block = weight[...] * gain[...]
    block = jnp.concatenate([block[:8], block[8:]], axis=1)
    gathered[z, x, y] = block.astype(jnp.bfloat16)
    pl.semaphore_wait(barrier, 34)
    along_y.start()
    ship(0, 0)

    def code_and_ship(p, carry):
        code(0, p, 0)
        return ship(p, carry)

    lax.fori_loop(1, FIRST, code_and_ship, 0)
    code_all(0, 4, 8, 1)
    code_all(1, 0, 4, 1)
    code_all(1, 4, 8, None)
    along_y.wait_recv()
    for copy in along_x:
        copy.start()

    group = lax.broadcasted_iota(jnp.int32, (8, 128), 1) // 32
    for q in range(8):
        blocks = [peaks[8 * k : 8 * k + 8, 0, 128 * q : 128 * q + 128] for k in range(4)]
        for r in range(4):
            turned = blocks[r]
            for k in range(4):
                if k != r:
                    turned = jnp.where(
                        group == k, pltpu.roll(blocks[k], (32 * (k - r)) % 128, 1), turned
                    )
            sent_side[4 * q + r] = turned.astype(jnp.bfloat16)
    landed_side[me] = sent_side[me]

    for peer in peers:
        pltpu.make_async_remote_copy(
            src_ref=sent_side.at[peer], dst_ref=landed_side.at[me],
            send_sem=side_send, recv_sem=side_recv,
            device_id=(own, peer), device_id_type=MESH,
        ).start()

    lax.fori_loop(FIRST, SECOND, ship, 0)

    def all_side():
        return pltpu.make_async_remote_copy(
            src_ref=sent_side.at[pl.ds(0, 31)], dst_ref=landed_side.at[pl.ds(0, 31)],
            send_sem=side_send, recv_sem=side_recv, device_id=(own, peers[0]), device_id_type=MESH,
        )

    def all_codes(c):
        return pltpu.make_async_remote_copy(
            src_ref=sent.at[c, pl.ds(0, 31)], dst_ref=landed.at[c, pl.ds(0, 31)],
            send_sem=send_sem, recv_sem=recv_sem.at[c],
            device_id=(own, peers[0]), device_id_type=MESH,
        )

    all_side().wait_recv()
    side[...] = landed_side[...].astype(jnp.float32)
    all_x.wait_recv()
    for copy in along_z:
        copy.start()
    lax.fori_loop(SECOND, THIRD, ship, 0)

    def pass_on(n, block, columns, to):
        return pltpu.make_async_remote_copy(
            src_ref=lines.at[block, :, columns], dst_ref=lines.at[block, :, columns],
            send_sem=line_send.at[n], recv_sem=line_recv.at[n],
            device_id=to, device_id_type=MESH,
        )

    whole = pl.ds(0, 2048)
    upward = pass_on(0, own, pl.ds(0, 1024), beside[0])
    downward = pass_on(1, own, pl.ds(1024, 1024), beside[1])
    over = pass_on(2, own, whole, beside[2])
    relay = pass_on(3, across, whole, beside[2])

    def pass_router():
        all_z.wait_recv()
        for k in range(16):
            pair = [
                gathered[k // 4, 2 * (k % 2) + h, (k // 2) % 2].astype(jnp.float32)
                for h in range(2)
            ]
            for h, block in enumerate(swap_halves(*pair)):
                lines[own, 8 * h : 8 * h + 8, 128 * k : 128 * k + 128] = block.astype(jnp.bfloat16)
        for copy in (upward, downward, over):
            copy.start()
        lax.fori_loop(THIRD, 16, ship, 0)

    at = lax.broadcasted_iota(jnp.int32, (32, 2048), 1) // 64
    picks = (at == lax.broadcasted_iota(jnp.int32, (32, 2048), 0)).astype(jnp.bfloat16)
    for r in range(8):
        turned = side[:, r, :].T.astype(jnp.bfloat16)
        spread[r] = jnp.dot(turned, picks, preferred_element_type=jnp.float32)

    scales[...] = jnp.zeros_like(scales)
    for m, out in enumerate((out_gate, out_up)):

        def decode(p, carry, m=m, out=out):
            c = 8 * m + p
            all_codes(c).wait_recv()
            rows = []
            for h in range(2):
                e = 2 * p + h
                rows.append((e % 8, pl.ds(pl.multiple_of(32 * (2 * m + e // 8), 32), 32)))
            sums = [jnp.zeros((32, 128), jnp.float32)] * 2
            for k in range(16):
                levels = []
                for s in range(2):
                    block = landed[c, 2 * k + s].astype(jnp.float32)
                    size = jnp.log2(jnp.abs(block)) + LOW
                    levels.append(jnp.where(block < 0, -size, size))
                for h, level in enumerate(swap_halves(*levels)):
                    f = level * spread[rows[h][0], rows[h][1], 128 * k : 128 * k + 128]
                    sums[h] += f * f
                    mixed[h, :, 128 * k : 128 * k + 128] = f
            lane = lax.broadcasted_iota(jnp.int32, (32, 128), 1)
            for h in range(2):
                e = 2 * p + h
                scale = jnp.sqrt(jnp.sum(sums[h], axis=1, keepdims=True))
                scales[...] = jnp.where(lane == 16 * m + e, scale * (1.0 / SPAN), scales[...])
                out[e] = (mixed[h] * (1.0 / scale)).astype(jnp.bfloat16)
            return carry

        if m == 0:
            lax.fori_loop(0, 6, decode, 0)
            pass_router()
            lax.fori_loop(6, 8, decode, 0)
        else:
            lax.fori_loop(0, 5, decode, 0)
            upward.wait_recv()
            downward.wait_recv()
            relay.start()
            lax.fori_loop(5, 8, decode, 0)

    turned = scales[...].T
    out_scale_gate[...] = turned[:16]
    out_scale_up[...] = turned[16:32]

    along_y.wait_send()
    all_x.wait_send()
    all_z.wait_send()
    over.wait()
    relay.wait()
    upward.wait_send()
    downward.wait_send()
    for o in range(4):
        out_router[16 * o : 16 * o + 16] = lines[o]

    all_side().wait_send()

    pltpu.make_async_remote_copy(
        src_ref=sent.at[:, pl.ds(0, 31)], dst_ref=landed.at[:, pl.ds(0, 31)],
        send_sem=send_sem, recv_sem=recv_sem.at[0],
        device_id=(own, peers[0]), device_id_type=MESH,
    ).wait_send()


def write_out(*refs):
    sems = refs[-1]
    n = (len(refs) - 1) // 2
    copies = [
        pltpu.make_async_copy(refs[i], refs[n + i], sems.at[i]) for i in range(n)
    ]
    for copy in copies:
        copy.start()
    for copy in copies:
        copy.wait()


def body(w_gate, avg_gate, w_up, avg_up, mix_share, router_weight, router_gain):
    vmem = pl.BlockSpec(memory_space=pltpu.VMEM)
    hbm = pl.BlockSpec(memory_space=pltpu.HBM)
    f32, bf16 = jnp.float32, jnp.bfloat16
    shapes = [
        ((16, 32, 2048), bf16),
        ((16, 32, 2048), bf16),
        ((16, 32), f32),
        ((16, 32), f32),
        ((64, 2048), bf16),
    ]
    results = pl.pallas_call(
        exchange,
        out_shape=[pltpu.VMEM(*shape) for shape in shapes],
        in_specs=[hbm] * 7,
        out_specs=[vmem] * 5,
        scratch_shapes=[
            pltpu.SMEM((16,), f32),
            pltpu.VMEM((16, 64), f32),
            pltpu.VMEM((1, 64), f32),
            pltpu.VMEM((2, 16, 64, 1024), f32),
            pltpu.VMEM((2, 16, 64, 1024), f32),
            pltpu.VMEM((32, 1, 1024), f32),
            pltpu.VMEM((16, 32, 32, 128), bf16),
            pltpu.VMEM((16, 32, 32, 128), bf16),
            pltpu.VMEM((32, 8, 128), bf16),
            pltpu.VMEM((32, 8, 128), bf16),
            pltpu.VMEM((32, 8, 128), f32),
            pltpu.VMEM((8, 128, 2048), f32),
            pltpu.VMEM((2, 32, 2048), f32),
            pltpu.VMEM((4, 4, 2, 8, 128), bf16),
            pltpu.VMEM((4, 16, 2048), bf16),
            pltpu.VMEM((32, 128), f32),
            pltpu.SemaphoreType.DMA((3,)),
            pltpu.SemaphoreType.DMA((AHEAD, 2)),
            pltpu.SemaphoreType.DMA,
            pltpu.SemaphoreType.DMA((16,)),
            pltpu.SemaphoreType.DMA,
            pltpu.SemaphoreType.DMA,
            pltpu.SemaphoreType.DMA((3,)),
            pltpu.SemaphoreType.DMA((3,)),
            pltpu.SemaphoreType.DMA((4,)),
            pltpu.SemaphoreType.DMA((4,)),
        ],
        compiler_params=pltpu.CompilerParams(
            collective_id=0, has_side_effects=True, vmem_limit_bytes=40 << 20
        ),
        name="exchange",
    )(
        *[
            pltpu.with_memory_space_constraint(a, pltpu.HBM)
            for a in (
                mix_share, w_gate, avg_gate, w_up, avg_up,
                router_weight.T, router_gain.reshape(1, 64),
            )
        ]
    )
    serve_gate, serve_up, scale_gate, scale_up, router = pl.pallas_call(
        write_out,
        out_shape=[jax.ShapeDtypeStruct(*shape) for shape in shapes],
        in_specs=[vmem] * 5,
        out_specs=[hbm] * 5,
        scratch_shapes=[pltpu.SemaphoreType.DMA((5,))],
        compiler_params=pltpu.CompilerParams(vmem_limit_bytes=4 << 20),
        name="write_out",
    )(*[pltpu.with_memory_space_constraint(a, pltpu.VMEM) for a in results])
    return (
        jnp.swapaxes(serve_gate, 1, 2),
        jnp.swapaxes(serve_up, 1, 2),
        scale_gate,
        scale_up,
        router.T,
    )


def solution(mesh):
    return jax.shard_map(
        body,
        mesh=mesh,
        in_specs=(
            P("owner", "rows", None),
            P("owner", "rows", None),
            P("owner", "rows", None),
            P("owner", "rows", None),
            P("owner"),
            P("rows", "owner"),
            P("rows"),
        ),
        out_specs=(
            P("owner", None, "rows"),
            P("owner", None, "rows"),
            P("owner", "rows"),
            P("owner", "rows"),
            P(),
        ),
        check_vma=False,
    )
```

```python
import functools

import jax
import jax.numpy as jnp
from jax import lax
from jax.experimental import pallas as pl
from jax.experimental.pallas import tpu as pltpu
from jax.sharding import PartitionSpec as P

MESH = pl.DeviceIdType.MESH
SPAN = 252.0
LOW = 125.0
AHEAD = 4
FIRST = 4
SECOND = 8
THIRD = 12
OFFSETS = [(a, b, c) for a in range(4) for b in range(2) for c in range(4)][1:]
FARTHEST = sorted(OFFSETS, key=lambda o: -min(o[0], 4 - o[0]) - 2 * o[1] - min(o[2], 4 - o[2]))


def left_half(shape):
    return lax.broadcasted_iota(jnp.int32, shape, len(shape) - 1) < 64


def swap_halves(a, b):
    left = left_half(a.shape)
    return jnp.where(left, a, pltpu.roll(b, 64, 1)), jnp.where(left, pltpu.roll(a, 64, 1), b)


def decode_pair(code, spread, mixed):
    sums = [jnp.zeros((32, 128), jnp.float32)] * 2
    for k in range(16):
        levels = []
        for s in range(2):
            block = code(2 * k + s).astype(jnp.float32)
            size = jnp.log2(jnp.abs(block)) + LOW
            levels.append(jnp.where(block < 0, -size, size))
        for h, level in enumerate(swap_halves(*levels)):
            f = level * spread(h, pl.ds(128 * k, 128))
            sums[h] += f * f
            mixed[h, :, 128 * k : 128 * k + 128] = f
    return [jnp.sqrt(jnp.sum(total, axis=1, keepdims=True)) for total in sums]


def exchange(
    mix_hbm, w_gate, v_gate, w_up, v_up, weight_hbm, gain_hbm,
    out_gate, out_up, out_router, scales, last_codes, last_spread,
    mix, weight, gain, w_in, v_in, peaks, sent, landed, sent_side, landed_side, side, spread, mixed, gathered, lines,
    small_sem, in_sem, send_sem, recv_sem, side_send, side_recv, gather_send, gather_recv, line_send, line_recv,
):
    me, own = lax.axis_index("rows"), lax.axis_index("owner")
    z, y, x = lax.div(me, 8), lax.rem(lax.div(me, 4), 2), lax.rem(me, 4)
    zs = [lax.rem(z + a, 4) * 8 for a in range(4)]
    ys = [y * 4, (1 - y) * 4]
    xs = [lax.rem(x + c, 4) for c in range(4)]
    peers = [zs[a] + ys[b] + xs[c] for a, b, c in FARTHEST]
    half = lax.div(own, 2)
    across = lax.rem(own + 2, 4)
    beside = [
        (across, z * 8 + lax.rem(y + half, 2) * 4 + x),
        (across, z * 8 + lax.rem(y + 1 - half, 2) * 4 + x),
        (own + 1 - 2 * lax.rem(own, 2), me),
    ]
    sources = ((w_gate, v_gate), (w_up, v_up))

    def arrival(m, p, k):
        return pltpu.make_async_copy(
            sources[m][k].at[pl.ds(2 * p, 2)],
            (w_in, v_in)[k].at[m, pl.ds(2 * p, 2)],
            in_sem.at[(p % AHEAD) if isinstance(p, int) else lax.rem(p, AHEAD), k],
        )

    barrier = pltpu.get_barrier_semaphore()
    for peer in peers:
        pl.semaphore_signal(barrier, inc=1, device_id=(own, peer), device_id_type=MESH)
    for other in beside:
        pl.semaphore_signal(barrier, inc=1, device_id=other, device_id_type=MESH)

    small = [
        pltpu.make_async_copy(a, b, small_sem.at[i])
        for i, (a, b) in enumerate(((mix_hbm, mix), (weight_hbm, weight), (gain_hbm, gain)))
    ]
    small[0].start()
    for p in range(AHEAD):
        for k in range(2):
            arrival(0, p, k).start()
    for copy in small[1:]:
        copy.start()

    small[0].wait()

    def code(m, p, ahead):
        for k in range(2):
            arrival(m, p, k).wait()
        if ahead is not None:
            for k in range(2):
                arrival(ahead, lax.rem(p + AHEAD, 8), k).start()
        for q in range(8):
            cols = pl.ds(128 * q, 128)
            halves = []
            for h in range(2):
                e = 2 * p + h
                share = mix[e]
                f = share * w_in[m, e, :, cols] + (1.0 - share) * v_in[m, e, :, cols]
                size = jnp.abs(f)
                peak = jnp.max(size, axis=0, keepdims=True)
                peak = (peak * (1.0 + 2.0**-7)).astype(jnp.bfloat16).astype(jnp.float32)
                peaks[16 * m + e, :, cols] = peak
                rate = jnp.where(peak > 1e-30, SPAN / peak, 0.0)
                level = jnp.exp2(size * rate - LOW)
                halves.append(jnp.where(f < 0, -level, level))
            block = jnp.concatenate(halves, axis=0).T.astype(jnp.bfloat16)
            for r in range(4):
                sent[8 * m + p, 4 * q + r] = block[32 * r : 32 * r + 32]
        landed[8 * m + p, me] = sent[8 * m + p, me]

    def code_all(m, begin, end, ahead):
        def step(p, carry):
            code(m, p, ahead)
            return carry

        lax.fori_loop(begin, end, step, 0)

    def gather(n, part, to):
        return pltpu.make_async_remote_copy(
            src_ref=part, dst_ref=part, send_sem=gather_send.at[n], recv_sem=gather_recv.at[n],
            device_id=(own, to), device_id_type=MESH,
        )

    along_y = gather(0, gathered.at[z, x, y], zs[0] + ys[1] + x)
    along_x = [gather(1, gathered.at[z, x], zs[0] + ys[0] + xs[c]) for c in (2, 1, 3)]
    along_z = [gather(2, gathered.at[z], zs[a] + ys[0] + x) for a in (2, 1, 3)]
    all_x = gather(1, gathered.at[0, pl.ds(0, 3)], peers[0])
    all_z = gather(2, gathered.at[pl.ds(0, 3)], peers[0])

    def ship(c, carry):
        for peer in peers:
            pltpu.make_async_remote_copy(
                src_ref=sent.at[c, peer], dst_ref=landed.at[c, me],
                send_sem=send_sem, recv_sem=recv_sem.at[c],
                device_id=(own, peer), device_id_type=MESH,
            ).start()
        return carry

    code_all(0, 0, 1, 0)
    for copy in small[1:]:
        copy.wait()
    block = weight[...] * gain[...]
    block = jnp.concatenate([block[:8], block[8:]], axis=1)
    gathered[z, x, y] = block.astype(jnp.bfloat16)
    pl.semaphore_wait(barrier, 34)
    along_y.start()
    ship(0, 0)

    def code_and_ship(p, carry):
        code(0, p, 0)
        return ship(p, carry)

    lax.fori_loop(1, FIRST, code_and_ship, 0)
    code_all(0, 4, 8, 1)
    code_all(1, 0, 4, 1)
    code_all(1, 4, 8, None)
    along_y.wait_recv()
    for copy in along_x:
        copy.start()

    group = lax.broadcasted_iota(jnp.int32, (8, 128), 1) // 32
    for q in range(8):
        blocks = [peaks[8 * k : 8 * k + 8, 0, 128 * q : 128 * q + 128] for k in range(4)]
        for r in range(4):
            turned = blocks[r]
            for k in range(4):
                if k != r:
                    turned = jnp.where(
                        group == k, pltpu.roll(blocks[k], (32 * (k - r)) % 128, 1), turned
                    )
            sent_side[4 * q + r] = turned.astype(jnp.bfloat16)
    landed_side[me] = sent_side[me]

    for peer in peers:
        pltpu.make_async_remote_copy(
            src_ref=sent_side.at[peer], dst_ref=landed_side.at[me],
            send_sem=side_send, recv_sem=side_recv,
            device_id=(own, peer), device_id_type=MESH,
        ).start()

    lax.fori_loop(FIRST, SECOND, ship, 0)

    def all_side():
        return pltpu.make_async_remote_copy(
            src_ref=sent_side.at[pl.ds(0, 31)], dst_ref=landed_side.at[pl.ds(0, 31)],
            send_sem=side_send, recv_sem=side_recv, device_id=(own, peers[0]), device_id_type=MESH,
        )

    def all_codes(c):
        return pltpu.make_async_remote_copy(
            src_ref=sent.at[c, pl.ds(0, 31)], dst_ref=landed.at[c, pl.ds(0, 31)],
            send_sem=send_sem, recv_sem=recv_sem.at[c],
            device_id=(own, peers[0]), device_id_type=MESH,
        )

    all_side().wait_recv()
    side[...] = landed_side[...].astype(jnp.float32)
    all_x.wait_recv()
    for copy in along_z:
        copy.start()
    lax.fori_loop(SECOND, THIRD, ship, 0)

    def pass_on(n, block, columns, to):
        return pltpu.make_async_remote_copy(
            src_ref=lines.at[block, :, columns], dst_ref=lines.at[block, :, columns],
            send_sem=line_send.at[n], recv_sem=line_recv.at[n],
            device_id=to, device_id_type=MESH,
        )

    whole = pl.ds(0, 2048)
    upward = pass_on(0, own, pl.ds(0, 1024), beside[0])
    downward = pass_on(1, own, pl.ds(1024, 1024), beside[1])
    over = pass_on(2, own, whole, beside[2])
    relay = pass_on(3, across, whole, beside[2])

    def pass_router():
        all_z.wait_recv()
        for k in range(16):
            pair = [
                gathered[k // 4, 2 * (k % 2) + h, (k // 2) % 2].astype(jnp.float32)
                for h in range(2)
            ]
            for h, block in enumerate(swap_halves(*pair)):
                lines[own, 8 * h : 8 * h + 8, 128 * k : 128 * k + 128] = block.astype(jnp.bfloat16)
        for copy in (upward, downward, over):
            copy.start()
        lax.fori_loop(THIRD, 16, ship, 0)

    at = lax.broadcasted_iota(jnp.int32, (32, 2048), 1) // 64
    picks = (at == lax.broadcasted_iota(jnp.int32, (32, 2048), 0)).astype(jnp.bfloat16)
    for r in range(8):
        turned = side[:, r, :].T.astype(jnp.bfloat16)
        spread[r] = jnp.dot(turned, picks, preferred_element_type=jnp.float32)

    def peak_rows(m, e):
        start = 32 * (2 * m + lax.div(e, 8))
        return lax.rem(e, 8), pl.ds(start if isinstance(start, int) else pl.multiple_of(start, 32), 32)

    for h in range(2):
        last_spread[h] = spread[6 + h, 96:128, :]

    scales[...] = jnp.zeros_like(scales)
    for m, out in enumerate((out_gate, out_up)):

        def decode(p, carry, m=m, out=out):
            c = 8 * m + p
            all_codes(c).wait_recv()
            found = decode_pair(
                lambda source: landed[c, source],
                lambda h, lanes: spread[peak_rows(m, 2 * p + h) + (lanes,)],
                mixed,
            )
            lane = lax.broadcasted_iota(jnp.int32, (32, 128), 1)
            for h, scale in enumerate(found):
                e = 2 * p + h
                scales[...] = jnp.where(lane == 16 * m + e, scale * (1.0 / SPAN), scales[...])
                out[e] = (mixed[h] * (1.0 / scale)).astype(jnp.bfloat16)
            return carry

        if m == 0:
            lax.fori_loop(0, 6, decode, 0)
            pass_router()
            lax.fori_loop(6, 8, decode, 0)
        else:
            lax.fori_loop(0, 5, decode, 0)
            upward.wait_recv()
            downward.wait_recv()
            relay.start()
            lax.fori_loop(5, 7, decode, 0)

    along_y.wait_send()
    all_x.wait_send()
    all_z.wait_send()
    over.wait()
    relay.wait()
    upward.wait_send()
    downward.wait_send()
    for o in range(4):
        out_router[16 * o : 16 * o + 16] = lines[o]

    all_side().wait_send()
    all_codes(15).wait_recv()
    last_codes[...] = landed[15]

    pltpu.make_async_remote_copy(
        src_ref=sent.at[:, pl.ds(0, 31)], dst_ref=landed.at[:, pl.ds(0, 31)],
        send_sem=send_sem, recv_sem=recv_sem.at[0],
        device_id=(own, peers[0]), device_id_type=MESH,
    ).wait_send()


def write_out(
    gate, up, router, scales, last_codes, last_spread,
    out_gate, out_up, out_scale_gate, out_scale_up, out_router,
    mixed, last, scale_gate, scale_up, sems,
):
    early = [(gate, out_gate), (up.at[:14], out_up.at[:14]), (router, out_router)]
    late = [(last, out_up.at[14:]), (scale_gate, out_scale_gate), (scale_up, out_scale_up)]
    copies = [pltpu.make_async_copy(a, b, sems.at[i]) for i, (a, b) in enumerate(early + late)]
    for copy in copies[:3]:
        copy.start()
    found = decode_pair(
        lambda source: last_codes[source], lambda h, lanes: last_spread[h, :, lanes], mixed
    )
    lane = lax.broadcasted_iota(jnp.int32, (32, 128), 1)
    table = scales[...]
    for h, scale in enumerate(found):
        table = jnp.where(lane == 30 + h, scale * (1.0 / SPAN), table)
        last[h] = (mixed[h] * (1.0 / scale)).astype(jnp.bfloat16)
    copies[3].start()
    turned = table.T
    scale_gate[...] = turned[:16]
    scale_up[...] = turned[16:32]
    for copy in copies[4:]:
        copy.start()
    for copy in copies:
        copy.wait()


def body(w_gate, avg_gate, w_up, avg_up, mix_share, router_weight, router_gain):
    vmem = pl.BlockSpec(memory_space=pltpu.VMEM)
    hbm = pl.BlockSpec(memory_space=pltpu.HBM)
    f32, bf16 = jnp.float32, jnp.bfloat16
    codes = [((16, 32, 2048), bf16), ((16, 32, 2048), bf16), ((64, 2048), bf16)]
    carried = codes + [((32, 128), f32), ((32, 32, 128), bf16), ((2, 32, 2048), f32)]
    shapes = codes[:2] + [((16, 32), f32), ((16, 32), f32), codes[2]]
    results = pl.pallas_call(
        exchange,
        out_shape=[pltpu.VMEM(*shape) for shape in carried],
        in_specs=[hbm] * 7,
        out_specs=[vmem] * 6,
        scratch_shapes=[
            pltpu.SMEM((16,), f32),
            pltpu.VMEM((16, 64), f32),
            pltpu.VMEM((1, 64), f32),
            pltpu.VMEM((2, 16, 64, 1024), f32),
            pltpu.VMEM((2, 16, 64, 1024), f32),
            pltpu.VMEM((32, 1, 1024), f32),
            pltpu.VMEM((16, 32, 32, 128), bf16),
            pltpu.VMEM((16, 32, 32, 128), bf16),
            pltpu.VMEM((32, 8, 128), bf16),
            pltpu.VMEM((32, 8, 128), bf16),
            pltpu.VMEM((32, 8, 128), f32),
            pltpu.VMEM((8, 128, 2048), f32),
            pltpu.VMEM((2, 32, 2048), f32),
            pltpu.VMEM((4, 4, 2, 8, 128), bf16),
            pltpu.VMEM((4, 16, 2048), bf16),
            pltpu.SemaphoreType.DMA((3,)),
            pltpu.SemaphoreType.DMA((AHEAD, 2)),
            pltpu.SemaphoreType.DMA,
            pltpu.SemaphoreType.DMA((16,)),
            pltpu.SemaphoreType.DMA,
            pltpu.SemaphoreType.DMA,
            pltpu.SemaphoreType.DMA((3,)),
            pltpu.SemaphoreType.DMA((3,)),
            pltpu.SemaphoreType.DMA((4,)),
            pltpu.SemaphoreType.DMA((4,)),
        ],
        compiler_params=pltpu.CompilerParams(
            collective_id=0, has_side_effects=True, vmem_limit_bytes=40 << 20
        ),
        name="exchange",
    )(
        *[
            pltpu.with_memory_space_constraint(a, pltpu.HBM)
            for a in (
                mix_share, w_gate, avg_gate, w_up, avg_up,
                router_weight.T, router_gain.reshape(1, 64),
            )
        ]
    )
    serve_gate, serve_up, scale_gate, scale_up, router = pl.pallas_call(
        write_out,
        out_shape=[jax.ShapeDtypeStruct(*shape) for shape in shapes],
        in_specs=[vmem] * 6,
        out_specs=[hbm] * 5,
        scratch_shapes=[
            pltpu.VMEM((2, 32, 2048), f32),
            pltpu.VMEM((2, 32, 2048), bf16),
            pltpu.VMEM((16, 32), f32),
            pltpu.VMEM((16, 32), f32),
            pltpu.SemaphoreType.DMA((6,)),
        ],
        compiler_params=pltpu.CompilerParams(vmem_limit_bytes=4 << 20),
        name="write_out",
    )(*[pltpu.with_memory_space_constraint(a, pltpu.VMEM) for a in results])
    return (
        jnp.swapaxes(serve_gate, 1, 2),
        jnp.swapaxes(serve_up, 1, 2),
        scale_gate,
        scale_up,
        router.T,
    )


def solution(mesh):
    return jax.shard_map(
        body,
        mesh=mesh,
        in_specs=(
            P("owner", "rows", None),
            P("owner", "rows", None),
            P("owner", "rows", None),
            P("owner", "rows", None),
            P("owner"),
            P("rows", "owner"),
            P("rows"),
        ),
        out_specs=(
            P("owner", None, "rows"),
            P("owner", None, "rows"),
            P("owner", "rows"),
            P("owner", "rows"),
            P(),
        ),
        check_vma=False,
    )
```

```python
import functools

import jax
import jax.numpy as jnp
from jax import lax
from jax.experimental import pallas as pl
from jax.experimental.pallas import tpu as pltpu
from jax.sharding import PartitionSpec as P

MESH = pl.DeviceIdType.MESH
SPAN = 252.0
LOW = 125.0
AHEAD = 4
FIRST = 4
SECOND = 8
THIRD = 12
LATE = 14
OFFSETS = [(a, b, c) for a in range(4) for b in range(2) for c in range(4)][1:]
FARTHEST = sorted(OFFSETS, key=lambda o: -min(o[0], 4 - o[0]) - 2 * o[1] - min(o[2], 4 - o[2]))


def left_half(shape):
    return lax.broadcasted_iota(jnp.int32, shape, len(shape) - 1) < 64


def swap_halves(a, b):
    left = left_half(a.shape)
    return jnp.where(left, a, pltpu.roll(b, 64, 1)), jnp.where(left, pltpu.roll(a, 64, 1), b)


def decode_pair(code, spread, mixed):
    sums = [jnp.zeros((32, 128), jnp.float32)] * 2
    for k in range(16):
        levels = []
        for s in range(2):
            block = code(2 * k + s).astype(jnp.float32)
            size = jnp.log2(jnp.abs(block)) + LOW
            levels.append(jnp.where(block < 0, -size, size))
        for h, level in enumerate(swap_halves(*levels)):
            f = level * spread(h, pl.ds(128 * k, 128))
            sums[h] += f * f
            mixed[h, :, 128 * k : 128 * k + 128] = f
    return [jnp.sqrt(jnp.sum(total, axis=1, keepdims=True)) for total in sums]


def exchange(
    mix_hbm, w_gate, v_gate, w_up, v_up, weight_hbm, gain_hbm,
    out_gate, out_up, out_router, scales, last_codes, last_spread,
    mix, weight, gain, w_in, v_in, peaks, sent, landed, sent_side, landed_side, side, spread, mixed, gathered, lines,
    small_sem, in_sem, send_sem, recv_sem, side_send, side_recv, gather_send, gather_recv, line_send, line_recv,
):
    me, own = lax.axis_index("rows"), lax.axis_index("owner")
    z, y, x = lax.div(me, 8), lax.rem(lax.div(me, 4), 2), lax.rem(me, 4)
    zs = [lax.rem(z + a, 4) * 8 for a in range(4)]
    ys = [y * 4, (1 - y) * 4]
    xs = [lax.rem(x + c, 4) for c in range(4)]
    peers = [zs[a] + ys[b] + xs[c] for a, b, c in FARTHEST]
    half = lax.div(own, 2)
    across = lax.rem(own + 2, 4)
    beside = [
        (across, z * 8 + lax.rem(y + half, 2) * 4 + x),
        (across, z * 8 + lax.rem(y + 1 - half, 2) * 4 + x),
        (own + 1 - 2 * lax.rem(own, 2), me),
    ]
    sources = ((w_gate, v_gate), (w_up, v_up))

    def arrival(m, p, k):
        return pltpu.make_async_copy(
            sources[m][k].at[pl.ds(2 * p, 2)],
            (w_in, v_in)[k].at[m, pl.ds(2 * p, 2)],
            in_sem.at[(p % AHEAD) if isinstance(p, int) else lax.rem(p, AHEAD), k],
        )

    barrier = pltpu.get_barrier_semaphore()
    for peer in peers:
        pl.semaphore_signal(barrier, inc=1, device_id=(own, peer), device_id_type=MESH)
    for other in beside:
        pl.semaphore_signal(barrier, inc=1, device_id=other, device_id_type=MESH)

    small = [
        pltpu.make_async_copy(a, b, small_sem.at[i])
        for i, (a, b) in enumerate(((mix_hbm, mix), (weight_hbm, weight), (gain_hbm, gain)))
    ]
    small[0].start()
    for p in range(AHEAD):
        for k in range(2):
            arrival(0, p, k).start()
    for copy in small[1:]:
        copy.start()

    small[0].wait()

    def code(m, p, ahead):
        for k in range(2):
            arrival(m, p, k).wait()
        if ahead is not None:
            for k in range(2):
                arrival(ahead, lax.rem(p + AHEAD, 8), k).start()
        for q in range(8):
            cols = pl.ds(128 * q, 128)
            halves = []
            for h in range(2):
                e = 2 * p + h
                share = mix[e]
                f = share * w_in[m, e, :, cols] + (1.0 - share) * v_in[m, e, :, cols]
                size = jnp.abs(f)
                peak = jnp.max(size, axis=0, keepdims=True)
                peak = (peak * (1.0 + 2.0**-7)).astype(jnp.bfloat16).astype(jnp.float32)
                peaks[16 * m + e, :, cols] = peak
                rate = jnp.where(peak > 1e-30, SPAN / peak, 0.0)
                level = jnp.exp2(size * rate - LOW)
                halves.append(jnp.where(f < 0, -level, level))
            block = jnp.concatenate(halves, axis=0).T.astype(jnp.bfloat16)
            for r in range(4):
                sent[8 * m + p, 4 * q + r] = block[32 * r : 32 * r + 32]
        landed[8 * m + p, me] = sent[8 * m + p, me]

    def code_all(m, begin, end, ahead):
        def step(p, carry):
            code(m, p, ahead)
            return carry

        lax.fori_loop(begin, end, step, 0)

    def gather(n, part, to):
        return pltpu.make_async_remote_copy(
            src_ref=part, dst_ref=part, send_sem=gather_send.at[n], recv_sem=gather_recv.at[n],
            device_id=(own, to), device_id_type=MESH,
        )

    along_y = gather(0, gathered.at[z, x, y], zs[0] + ys[1] + x)
    along_x = [gather(1, gathered.at[z, x], zs[0] + ys[0] + xs[c]) for c in (2, 1, 3)]
    along_z = [gather(2, gathered.at[z], zs[a] + ys[0] + x) for a in (2, 1, 3)]
    all_x = gather(1, gathered.at[0, pl.ds(0, 3)], peers[0])
    all_z = gather(2, gathered.at[pl.ds(0, 3)], peers[0])

    def ship(c, carry):
        for peer in peers:
            pltpu.make_async_remote_copy(
                src_ref=sent.at[c, peer], dst_ref=landed.at[c, me],
                send_sem=send_sem, recv_sem=recv_sem.at[c],
                device_id=(own, peer), device_id_type=MESH,
            ).start()
        return carry

    code_all(0, 0, 1, 0)
    for copy in small[1:]:
        copy.wait()
    block = weight[...] * gain[...]
    block = jnp.concatenate([block[:8], block[8:]], axis=1)
    gathered[z, x, y] = block.astype(jnp.bfloat16)
    pl.semaphore_wait(barrier, 34)
    along_y.start()
    ship(0, 0)

    def code_and_ship(p, carry):
        code(0, p, 0)
        return ship(p, carry)

    lax.fori_loop(1, FIRST, code_and_ship, 0)
    code_all(0, 4, 8, 1)
    code_all(1, 0, 4, 1)
    code_all(1, 4, 8, None)
    along_y.wait_recv()
    for copy in along_x:
        copy.start()

    group = lax.broadcasted_iota(jnp.int32, (8, 128), 1) // 32
    for q in range(8):
        blocks = [peaks[8 * k : 8 * k + 8, 0, 128 * q : 128 * q + 128] for k in range(4)]
        for r in range(4):
            turned = blocks[r]
            for k in range(4):
                if k != r:
                    turned = jnp.where(
                        group == k, pltpu.roll(blocks[k], (32 * (k - r)) % 128, 1), turned
                    )
            sent_side[4 * q + r] = turned.astype(jnp.bfloat16)
    landed_side[me] = sent_side[me]

    for peer in peers:
        pltpu.make_async_remote_copy(
            src_ref=sent_side.at[peer], dst_ref=landed_side.at[me],
            send_sem=side_send, recv_sem=side_recv,
            device_id=(own, peer), device_id_type=MESH,
        ).start()

    lax.fori_loop(FIRST, SECOND, ship, 0)

    def all_side():
        return pltpu.make_async_remote_copy(
            src_ref=sent_side.at[pl.ds(0, 31)], dst_ref=landed_side.at[pl.ds(0, 31)],
            send_sem=side_send, recv_sem=side_recv, device_id=(own, peers[0]), device_id_type=MESH,
        )

    def all_codes(c):
        return pltpu.make_async_remote_copy(
            src_ref=sent.at[c, pl.ds(0, 31)], dst_ref=landed.at[c, pl.ds(0, 31)],
            send_sem=send_sem, recv_sem=recv_sem.at[c],
            device_id=(own, peers[0]), device_id_type=MESH,
        )

    all_side().wait_recv()
    side[...] = landed_side[...].astype(jnp.float32)
    all_x.wait_recv()
    for copy in along_z:
        copy.start()
    lax.fori_loop(SECOND, THIRD, ship, 0)

    def pass_on(n, block, columns, to):
        return pltpu.make_async_remote_copy(
            src_ref=lines.at[block, :, columns], dst_ref=lines.at[block, :, columns],
            send_sem=line_send.at[n], recv_sem=line_recv.at[n],
            device_id=to, device_id_type=MESH,
        )

    whole = pl.ds(0, 2048)
    upward = pass_on(0, own, pl.ds(0, 1024), beside[0])
    downward = pass_on(1, own, pl.ds(1024, 1024), beside[1])
    over = pass_on(2, own, whole, beside[2])
    relay = pass_on(3, across, whole, beside[2])

    def pass_router():
        all_z.wait_recv()
        for k in range(16):
            pair = [
                gathered[k // 4, 2 * (k % 2) + h, (k // 2) % 2].astype(jnp.float32)
                for h in range(2)
            ]
            for h, block in enumerate(swap_halves(*pair)):
                lines[own, 8 * h : 8 * h + 8, 128 * k : 128 * k + 128] = block.astype(jnp.bfloat16)
        for copy in (upward, downward, over):
            copy.start()
        lax.fori_loop(THIRD, LATE, ship, 0)
        for peer in peers:
            for c in range(LATE, 16):
                pltpu.make_async_remote_copy(
                    src_ref=sent.at[c, peer], dst_ref=landed.at[c, me],
                    send_sem=send_sem, recv_sem=recv_sem.at[c],
                    device_id=(own, peer), device_id_type=MESH,
                ).start()

    at = lax.broadcasted_iota(jnp.int32, (32, 2048), 1) // 64
    picks = (at == lax.broadcasted_iota(jnp.int32, (32, 2048), 0)).astype(jnp.bfloat16)
    for r in range(8):
        turned = side[:, r, :].T.astype(jnp.bfloat16)
        spread[r] = jnp.dot(turned, picks, preferred_element_type=jnp.float32)

    def peak_rows(m, e):
        start = 32 * (2 * m + lax.div(e, 8))
        return lax.rem(e, 8), pl.ds(start if isinstance(start, int) else pl.multiple_of(start, 32), 32)

    for h in range(4):
        last_spread[h] = spread[4 + h, 96:128, :]

    scales[...] = jnp.zeros_like(scales)
    for m, out in enumerate((out_gate, out_up)):

        def decode(p, carry, m=m, out=out):
            c = 8 * m + p
            all_codes(c).wait_recv()
            found = decode_pair(
                lambda source: landed[c, source],
                lambda h, lanes: spread[peak_rows(m, 2 * p + h) + (lanes,)],
                mixed,
            )
            lane = lax.broadcasted_iota(jnp.int32, (32, 128), 1)
            for h, scale in enumerate(found):
                e = 2 * p + h
                scales[...] = jnp.where(lane == 16 * m + e, scale * (1.0 / SPAN), scales[...])
                out[e] = (mixed[h] * (1.0 / scale)).astype(jnp.bfloat16)
            return carry

        if m == 0:
            lax.fori_loop(0, 6, decode, 0)
            pass_router()
            lax.fori_loop(6, 8, decode, 0)
        else:
            lax.fori_loop(0, 5, decode, 0)
            upward.wait_recv()
            downward.wait_recv()
            relay.start()
            lax.fori_loop(5, 6, decode, 0)

    along_y.wait_send()
    all_x.wait_send()
    all_z.wait_send()
    over.wait()
    relay.wait()
    upward.wait_send()
    downward.wait_send()
    for o in range(4):
        out_router[16 * o : 16 * o + 16] = lines[o]

    all_side().wait_send()
    for c in range(LATE, 16):
        all_codes(c).wait_recv()
        last_codes[c - LATE] = landed[c]

    pltpu.make_async_remote_copy(
        src_ref=sent.at[:, pl.ds(0, 31)], dst_ref=landed.at[:, pl.ds(0, 31)],
        send_sem=send_sem, recv_sem=recv_sem.at[0],
        device_id=(own, peers[0]), device_id_type=MESH,
    ).wait_send()


def write_out(
    gate, up, router, scales, last_codes, last_spread,
    out_gate, out_up, out_scale_gate, out_scale_up, out_router,
    mixed, last, scale_gate, scale_up, sems,
):
    early = [(gate, out_gate), (up.at[:12], out_up.at[:12]), (router, out_router)]
    late = [(last.at[2 * n : 2 * n + 2], out_up.at[12 + 2 * n : 14 + 2 * n]) for n in range(2)]
    late += [(scale_gate, out_scale_gate), (scale_up, out_scale_up)]
    copies = [pltpu.make_async_copy(a, b, sems.at[i]) for i, (a, b) in enumerate(early + late)]
    for copy in copies[:3]:
        copy.start()
    lane = lax.broadcasted_iota(jnp.int32, (32, 128), 1)
    table = scales[...]
    for n in range(2):
        found = decode_pair(
            lambda source: last_codes[n, source],
            lambda h, lanes: last_spread[2 * n + h, :, lanes],
            mixed,
        )
        for h, scale in enumerate(found):
            table = jnp.where(lane == 28 + 2 * n + h, scale * (1.0 / SPAN), table)
            last[2 * n + h] = (mixed[h] * (1.0 / scale)).astype(jnp.bfloat16)
        copies[3 + n].start()
    turned = table.T
    scale_gate[...] = turned[:16]
    scale_up[...] = turned[16:32]
    for copy in copies[5:]:
        copy.start()
    for copy in copies:
        copy.wait()


def body(w_gate, avg_gate, w_up, avg_up, mix_share, router_weight, router_gain):
    vmem = pl.BlockSpec(memory_space=pltpu.VMEM)
    hbm = pl.BlockSpec(memory_space=pltpu.HBM)
    f32, bf16 = jnp.float32, jnp.bfloat16
    codes = [((16, 32, 2048), bf16), ((16, 32, 2048), bf16), ((64, 2048), bf16)]
    carried = codes + [((32, 128), f32), ((2, 32, 32, 128), bf16), ((4, 32, 2048), f32)]
    shapes = codes[:2] + [((16, 32), f32), ((16, 32), f32), codes[2]]
    results = pl.pallas_call(
        exchange,
        out_shape=[pltpu.VMEM(*shape) for shape in carried],
        in_specs=[hbm] * 7,
        out_specs=[vmem] * 6,
        scratch_shapes=[
            pltpu.SMEM((16,), f32),
            pltpu.VMEM((16, 64), f32),
            pltpu.VMEM((1, 64), f32),
            pltpu.VMEM((2, 16, 64, 1024), f32),
            pltpu.VMEM((2, 16, 64, 1024), f32),
            pltpu.VMEM((32, 1, 1024), f32),
            pltpu.VMEM((16, 32, 32, 128), bf16),
            pltpu.VMEM((16, 32, 32, 128), bf16),
            pltpu.VMEM((32, 8, 128), bf16),
            pltpu.VMEM((32, 8, 128), bf16),
            pltpu.VMEM((32, 8, 128), f32),
            pltpu.VMEM((8, 128, 2048), f32),
            pltpu.VMEM((2, 32, 2048), f32),
            pltpu.VMEM((4, 4, 2, 8, 128), bf16),
            pltpu.VMEM((4, 16, 2048), bf16),
            pltpu.SemaphoreType.DMA((3,)),
            pltpu.SemaphoreType.DMA((AHEAD, 2)),
            pltpu.SemaphoreType.DMA,
            pltpu.SemaphoreType.DMA((16,)),
            pltpu.SemaphoreType.DMA,
            pltpu.SemaphoreType.DMA,
            pltpu.SemaphoreType.DMA((3,)),
            pltpu.SemaphoreType.DMA((3,)),
            pltpu.SemaphoreType.DMA((4,)),
            pltpu.SemaphoreType.DMA((4,)),
        ],
        compiler_params=pltpu.CompilerParams(
            collective_id=0, has_side_effects=True, vmem_limit_bytes=40 << 20
        ),
        name="exchange",
    )(
        *[
            pltpu.with_memory_space_constraint(a, pltpu.HBM)
            for a in (
                mix_share, w_gate, avg_gate, w_up, avg_up,
                router_weight.T, router_gain.reshape(1, 64),
            )
        ]
    )
    serve_gate, serve_up, scale_gate, scale_up, router = pl.pallas_call(
        write_out,
        out_shape=[jax.ShapeDtypeStruct(*shape) for shape in shapes],
        in_specs=[vmem] * 6,
        out_specs=[hbm] * 5,
        scratch_shapes=[
            pltpu.VMEM((2, 32, 2048), f32),
            pltpu.VMEM((4, 32, 2048), bf16),
            pltpu.VMEM((16, 32), f32),
            pltpu.VMEM((16, 32), f32),
            pltpu.SemaphoreType.DMA((7,)),
        ],
        compiler_params=pltpu.CompilerParams(vmem_limit_bytes=4 << 20),
        name="write_out",
    )(*[pltpu.with_memory_space_constraint(a, pltpu.VMEM) for a in results])
    return (
        jnp.swapaxes(serve_gate, 1, 2),
        jnp.swapaxes(serve_up, 1, 2),
        scale_gate,
        scale_up,
        router.T,
    )


def solution(mesh):
    return jax.shard_map(
        body,
        mesh=mesh,
        in_specs=(
            P("owner", "rows", None),
            P("owner", "rows", None),
            P("owner", "rows", None),
            P("owner", "rows", None),
            P("owner"),
            P("rows", "owner"),
            P("rows"),
        ),
        out_specs=(
            P("owner", None, "rows"),
            P("owner", None, "rows"),
            P("owner", "rows"),
            P("owner", "rows"),
            P(),
        ),
        check_vma=False,
    )
```

```python
import functools

import jax
import jax.numpy as jnp
from jax import lax
from jax.experimental import pallas as pl
from jax.experimental.pallas import tpu as pltpu
from jax.sharding import PartitionSpec as P

MESH = pl.DeviceIdType.MESH
SPAN = 252.0
LOW = 125.0
AHEAD = 4
FIRST = 4
SECOND = 8
THIRD = 12
LATE = 14
OFFSETS = [(a, b, c) for a in range(4) for b in range(2) for c in range(4)][1:]
FARTHEST = sorted(OFFSETS, key=lambda o: -min(o[0], 4 - o[0]) - 8 * o[1] - min(o[2], 4 - o[2]))


def left_half(shape):
    return lax.broadcasted_iota(jnp.int32, shape, len(shape) - 1) < 64


def swap_halves(a, b):
    left = left_half(a.shape)
    return jnp.where(left, a, pltpu.roll(b, 64, 1)), jnp.where(left, pltpu.roll(a, 64, 1), b)


def decode_pair(code, spread, mixed):
    sums = [jnp.zeros((32, 128), jnp.float32)] * 2
    for k in range(16):
        levels = []
        for s in range(2):
            block = code(2 * k + s).astype(jnp.float32)
            size = jnp.log2(jnp.abs(block)) + LOW
            levels.append(jnp.where(block < 0, -size, size))
        for h, level in enumerate(swap_halves(*levels)):
            f = level * spread(h, pl.ds(128 * k, 128))
            sums[h] += f * f
            mixed[h, :, 128 * k : 128 * k + 128] = f
    return [jnp.sqrt(jnp.sum(total, axis=1, keepdims=True)) for total in sums]


def exchange(
    mix_hbm, w_gate, v_gate, w_up, v_up, weight_hbm, gain_hbm,
    out_gate, out_up, out_router, scales, last_codes, last_spread,
    mix, weight, gain, w_in, v_in, peaks, sent, landed, sent_side, landed_side, side, spread, mixed, gathered, lines,
    small_sem, in_sem, send_sem, recv_sem, side_send, side_recv, gather_send, gather_recv, line_send, line_recv,
):
    me, own = lax.axis_index("rows"), lax.axis_index("owner")
    z, y, x = lax.div(me, 8), lax.rem(lax.div(me, 4), 2), lax.rem(me, 4)
    zs = [lax.rem(z + a, 4) * 8 for a in range(4)]
    ys = [y * 4, (1 - y) * 4]
    xs = [lax.rem(x + c, 4) for c in range(4)]
    peers = [zs[a] + ys[b] + xs[c] for a, b, c in FARTHEST]
    half = lax.div(own, 2)
    across = lax.rem(own + 2, 4)
    beside = [
        (across, z * 8 + lax.rem(y + half, 2) * 4 + x),
        (across, z * 8 + lax.rem(y + 1 - half, 2) * 4 + x),
        (own + 1 - 2 * lax.rem(own, 2), me),
    ]
    sources = ((w_gate, v_gate), (w_up, v_up))

    def arrival(m, p, k):
        return pltpu.make_async_copy(
            sources[m][k].at[pl.ds(2 * p, 2)],
            (w_in, v_in)[k].at[m, pl.ds(2 * p, 2)],
            in_sem.at[(p % AHEAD) if isinstance(p, int) else lax.rem(p, AHEAD), k],
        )

    barrier = pltpu.get_barrier_semaphore()
    for peer in peers:
        pl.semaphore_signal(barrier, inc=1, device_id=(own, peer), device_id_type=MESH)
    for other in beside:
        pl.semaphore_signal(barrier, inc=1, device_id=other, device_id_type=MESH)

    small = [
        pltpu.make_async_copy(a, b, small_sem.at[i])
        for i, (a, b) in enumerate(((mix_hbm, mix), (weight_hbm, weight), (gain_hbm, gain)))
    ]
    small[0].start()
    for p in range(AHEAD):
        for k in range(2):
            arrival(0, p, k).start()
    for copy in small[1:]:
        copy.start()

    small[0].wait()

    def code(m, p, ahead):
        for k in range(2):
            arrival(m, p, k).wait()
        if ahead is not None:
            for k in range(2):
                arrival(ahead, lax.rem(p + AHEAD, 8), k).start()
        for q in range(8):
            cols = pl.ds(128 * q, 128)
            halves = []
            for h in range(2):
                e = 2 * p + h
                share = mix[e]
                f = share * w_in[m, e, :, cols] + (1.0 - share) * v_in[m, e, :, cols]
                size = jnp.abs(f)
                peak = jnp.max(size, axis=0, keepdims=True)
                peak = (peak * (1.0 + 2.0**-7)).astype(jnp.bfloat16).astype(jnp.float32)
                peaks[16 * m + e, :, cols] = peak
                rate = jnp.where(peak > 1e-30, SPAN / peak, 0.0)
                level = jnp.exp2(size * rate - LOW)
                halves.append(jnp.where(f < 0, -level, level))
            block = jnp.concatenate(halves, axis=0).T.astype(jnp.bfloat16)
            for r in range(4):
                sent[8 * m + p, 4 * q + r] = block[32 * r : 32 * r + 32]
        landed[8 * m + p, me] = sent[8 * m + p, me]

    def code_all(m, begin, end, ahead):
        def step(p, carry):
            code(m, p, ahead)
            return carry

        lax.fori_loop(begin, end, step, 0)

    def gather(n, part, to):
        return pltpu.make_async_remote_copy(
            src_ref=part, dst_ref=part, send_sem=gather_send.at[n], recv_sem=gather_recv.at[n],
            device_id=(own, to), device_id_type=MESH,
        )

    along_y = gather(0, gathered.at[z, x, y], zs[0] + ys[1] + x)
    along_x = [gather(1, gathered.at[z, x], zs[0] + ys[0] + xs[c]) for c in (2, 1, 3)]
    along_z = [gather(2, gathered.at[z], zs[a] + ys[0] + x) for a in (2, 1, 3)]
    all_x = gather(1, gathered.at[0, pl.ds(0, 3)], peers[0])
    all_z = gather(2, gathered.at[pl.ds(0, 3)], peers[0])

    def ship(c, carry):
        for peer in peers:
            pltpu.make_async_remote_copy(
                src_ref=sent.at[c, peer], dst_ref=landed.at[c, me],
                send_sem=send_sem, recv_sem=recv_sem.at[c],
                device_id=(own, peer), device_id_type=MESH,
            ).start()
        return carry

    code_all(0, 0, 1, 0)
    for copy in small[1:]:
        copy.wait()
    block = weight[...] * gain[...]
    block = jnp.concatenate([block[:8], block[8:]], axis=1)
    gathered[z, x, y] = block.astype(jnp.bfloat16)
    pl.semaphore_wait(barrier, 34)
    along_y.start()
    ship(0, 0)

    def code_and_ship(p, carry):
        code(0, p, 0)
        return ship(p, carry)

    lax.fori_loop(1, FIRST, code_and_ship, 0)
    code_all(0, 4, 8, 1)
    code_all(1, 0, 4, 1)
    code_all(1, 4, 8, None)
    along_y.wait_recv()
    for copy in along_x:
        copy.start()

    group = lax.broadcasted_iota(jnp.int32, (8, 128), 1) // 32
    for q in range(8):
        blocks = [peaks[8 * k : 8 * k + 8, 0, 128 * q : 128 * q + 128] for k in range(4)]
        for r in range(4):
            turned = blocks[r]
            for k in range(4):
                if k != r:
                    turned = jnp.where(
                        group == k, pltpu.roll(blocks[k], (32 * (k - r)) % 128, 1), turned
                    )
            sent_side[4 * q + r] = turned.astype(jnp.bfloat16)
    landed_side[me] = sent_side[me]

    for peer in peers:
        pltpu.make_async_remote_copy(
            src_ref=sent_side.at[peer], dst_ref=landed_side.at[me],
            send_sem=side_send, recv_sem=side_recv,
            device_id=(own, peer), device_id_type=MESH,
        ).start()

    lax.fori_loop(FIRST, SECOND, ship, 0)

    def all_side():
        return pltpu.make_async_remote_copy(
            src_ref=sent_side.at[pl.ds(0, 31)], dst_ref=landed_side.at[pl.ds(0, 31)],
            send_sem=side_send, recv_sem=side_recv, device_id=(own, peers[0]), device_id_type=MESH,
        )

    def all_codes(c):
        return pltpu.make_async_remote_copy(
            src_ref=sent.at[c, pl.ds(0, 31)], dst_ref=landed.at[c, pl.ds(0, 31)],
            send_sem=send_sem, recv_sem=recv_sem.at[c],
            device_id=(own, peers[0]), device_id_type=MESH,
        )

    all_side().wait_recv()
    side[...] = landed_side[...].astype(jnp.float32)
    all_x.wait_recv()
    for copy in along_z:
        copy.start()
    lax.fori_loop(SECOND, THIRD, ship, 0)

    def pass_on(n, block, columns, to):
        return pltpu.make_async_remote_copy(
            src_ref=lines.at[block, :, columns], dst_ref=lines.at[block, :, columns],
            send_sem=line_send.at[n], recv_sem=line_recv.at[n],
            device_id=to, device_id_type=MESH,
        )

    whole = pl.ds(0, 2048)
    upward = pass_on(0, own, pl.ds(0, 1024), beside[0])
    downward = pass_on(1, own, pl.ds(1024, 1024), beside[1])
    over = pass_on(2, own, whole, beside[2])
    relay = pass_on(3, across, whole, beside[2])

    def pass_router():
        all_z.wait_recv()
        for k in range(16):
            pair = [
                gathered[k // 4, 2 * (k % 2) + h, (k // 2) % 2].astype(jnp.float32)
                for h in range(2)
            ]
            for h, block in enumerate(swap_halves(*pair)):
                lines[own, 8 * h : 8 * h + 8, 128 * k : 128 * k + 128] = block.astype(jnp.bfloat16)
        for copy in (upward, downward, over):
            copy.start()
        lax.fori_loop(THIRD, LATE, ship, 0)
        for peer in peers:
            for c in range(LATE, 16):
                pltpu.make_async_remote_copy(
                    src_ref=sent.at[c, peer], dst_ref=landed.at[c, me],
                    send_sem=send_sem, recv_sem=recv_sem.at[c],
                    device_id=(own, peer), device_id_type=MESH,
                ).start()

    at = lax.broadcasted_iota(jnp.int32, (32, 2048), 1) // 64
    picks = (at == lax.broadcasted_iota(jnp.int32, (32, 2048), 0)).astype(jnp.bfloat16)
    for r in range(8):
        turned = side[:, r, :].T.astype(jnp.bfloat16)
        spread[r] = jnp.dot(turned, picks, preferred_element_type=jnp.float32)

    def peak_rows(m, e):
        start = 32 * (2 * m + lax.div(e, 8))
        return lax.rem(e, 8), pl.ds(start if isinstance(start, int) else pl.multiple_of(start, 32), 32)

    for h in range(4):
        last_spread[h] = spread[4 + h, 96:128, :]

    scales[...] = jnp.zeros_like(scales)
    for m, out in enumerate((out_gate, out_up)):

        def decode(p, carry, m=m, out=out):
            c = 8 * m + p
            all_codes(c).wait_recv()
            found = decode_pair(
                lambda source: landed[c, source],
                lambda h, lanes: spread[peak_rows(m, 2 * p + h) + (lanes,)],
                mixed,
            )
            lane = lax.broadcasted_iota(jnp.int32, (32, 128), 1)
            for h, scale in enumerate(found):
                e = 2 * p + h
                scales[...] = jnp.where(lane == 16 * m + e, scale * (1.0 / SPAN), scales[...])
                out[e] = (mixed[h] * (1.0 / scale)).astype(jnp.bfloat16)
            return carry

        if m == 0:
            lax.fori_loop(0, 6, decode, 0)
            pass_router()
            lax.fori_loop(6, 8, decode, 0)
        else:
            lax.fori_loop(0, 5, decode, 0)
            upward.wait_recv()
            downward.wait_recv()
            relay.start()
            lax.fori_loop(5, 6, decode, 0)

    along_y.wait_send()
    all_x.wait_send()
    all_z.wait_send()
    over.wait()
    relay.wait()
    upward.wait_send()
    downward.wait_send()
    for o in range(4):
        out_router[16 * o : 16 * o + 16] = lines[o]

    all_side().wait_send()
    for c in range(LATE, 16):
        all_codes(c).wait_recv()
        last_codes[c - LATE] = landed[c]

    pltpu.make_async_remote_copy(
        src_ref=sent.at[:, pl.ds(0, 31)], dst_ref=landed.at[:, pl.ds(0, 31)],
        send_sem=send_sem, recv_sem=recv_sem.at[0],
        device_id=(own, peers[0]), device_id_type=MESH,
    ).wait_send()


def write_out(
    gate, up, router, scales, last_codes, last_spread,
    out_gate, out_up, out_scale_gate, out_scale_up, out_router,
    mixed, last, scale_gate, scale_up, sems,
):
    early = [(gate, out_gate), (up.at[:12], out_up.at[:12]), (router, out_router)]
    late = [(last.at[2 * n : 2 * n + 2], out_up.at[12 + 2 * n : 14 + 2 * n]) for n in range(2)]
    late += [(scale_gate, out_scale_gate), (scale_up, out_scale_up)]
    copies = [pltpu.make_async_copy(a, b, sems.at[i]) for i, (a, b) in enumerate(early + late)]
    for copy in copies[:3]:
        copy.start()
    lane = lax.broadcasted_iota(jnp.int32, (32, 128), 1)
    table = scales[...]
    for n in range(2):
        found = decode_pair(
            lambda source: last_codes[n, source],
            lambda h, lanes: last_spread[2 * n + h, :, lanes],
            mixed,
        )
        for h, scale in enumerate(found):
            table = jnp.where(lane == 28 + 2 * n + h, scale * (1.0 / SPAN), table)
            last[2 * n + h] = (mixed[h] * (1.0 / scale)).astype(jnp.bfloat16)
        copies[3 + n].start()
    turned = table.T
    scale_gate[...] = turned[:16]
    scale_up[...] = turned[16:32]
    for copy in copies[5:]:
        copy.start()
    for copy in copies:
        copy.wait()


def body(w_gate, avg_gate, w_up, avg_up, mix_share, router_weight, router_gain):
    vmem = pl.BlockSpec(memory_space=pltpu.VMEM)
    hbm = pl.BlockSpec(memory_space=pltpu.HBM)
    f32, bf16 = jnp.float32, jnp.bfloat16
    codes = [((16, 32, 2048), bf16), ((16, 32, 2048), bf16), ((64, 2048), bf16)]
    carried = codes + [((32, 128), f32), ((2, 32, 32, 128), bf16), ((4, 32, 2048), f32)]
    shapes = codes[:2] + [((16, 32), f32), ((16, 32), f32), codes[2]]
    results = pl.pallas_call(
        exchange,
        out_shape=[pltpu.VMEM(*shape) for shape in carried],
        in_specs=[hbm] * 7,
        out_specs=[vmem] * 6,
        scratch_shapes=[
            pltpu.SMEM((16,), f32),
            pltpu.VMEM((16, 64), f32),
            pltpu.VMEM((1, 64), f32),
            pltpu.VMEM((2, 16, 64, 1024), f32),
            pltpu.VMEM((2, 16, 64, 1024), f32),
            pltpu.VMEM((32, 1, 1024), f32),
            pltpu.VMEM((16, 32, 32, 128), bf16),
            pltpu.VMEM((16, 32, 32, 128), bf16),
            pltpu.VMEM((32, 8, 128), bf16),
            pltpu.VMEM((32, 8, 128), bf16),
            pltpu.VMEM((32, 8, 128), f32),
            pltpu.VMEM((8, 128, 2048), f32),
            pltpu.VMEM((2, 32, 2048), f32),
            pltpu.VMEM((4, 4, 2, 8, 128), bf16),
            pltpu.VMEM((4, 16, 2048), bf16),
            pltpu.SemaphoreType.DMA((3,)),
            pltpu.SemaphoreType.DMA((AHEAD, 2)),
            pltpu.SemaphoreType.DMA,
            pltpu.SemaphoreType.DMA((16,)),
            pltpu.SemaphoreType.DMA,
            pltpu.SemaphoreType.DMA,
            pltpu.SemaphoreType.DMA((3,)),
            pltpu.SemaphoreType.DMA((3,)),
            pltpu.SemaphoreType.DMA((4,)),
            pltpu.SemaphoreType.DMA((4,)),
        ],
        compiler_params=pltpu.CompilerParams(
            collective_id=0, has_side_effects=True, vmem_limit_bytes=40 << 20
        ),
        name="exchange",
    )(
        *[
            pltpu.with_memory_space_constraint(a, pltpu.HBM)
            for a in (
                mix_share, w_gate, avg_gate, w_up, avg_up,
                router_weight.T, router_gain.reshape(1, 64),
            )
        ]
    )
    serve_gate, serve_up, scale_gate, scale_up, router = pl.pallas_call(
        write_out,
        out_shape=[jax.ShapeDtypeStruct(*shape) for shape in shapes],
        in_specs=[vmem] * 6,
        out_specs=[hbm] * 5,
        scratch_shapes=[
            pltpu.VMEM((2, 32, 2048), f32),
            pltpu.VMEM((4, 32, 2048), bf16),
            pltpu.VMEM((16, 32), f32),
            pltpu.VMEM((16, 32), f32),
            pltpu.SemaphoreType.DMA((7,)),
        ],
        compiler_params=pltpu.CompilerParams(vmem_limit_bytes=4 << 20),
        name="write_out",
    )(*[pltpu.with_memory_space_constraint(a, pltpu.VMEM) for a in results])
    return (
        jnp.swapaxes(serve_gate, 1, 2),
        jnp.swapaxes(serve_up, 1, 2),
        scale_gate,
        scale_up,
        router.T,
    )


def solution(mesh):
    return jax.shard_map(
        body,
        mesh=mesh,
        in_specs=(
            P("owner", "rows", None),
            P("owner", "rows", None),
            P("owner", "rows", None),
            P("owner", "rows", None),
            P("owner"),
            P("rows", "owner"),
            P("rows"),
        ),
        out_specs=(
            P("owner", None, "rows"),
            P("owner", None, "rows"),
            P("owner", "rows"),
            P("owner", "rows"),
            P(),
        ),
        check_vma=False,
    )
```
